256 devices in a mesh: dp: 128 (over z, x, y_lo, core), tp: 2 (over y_hi).
Axes of the slice: x: 4, y: 4 (y_hi: 2, y_lo: 2; y = y_hi * 2 + y_lo), z: 8, core: 2. Of those that a mesh axis runs over, the one named last changes fastest.
Arguments:
- q_nope: bfloat16 [4096, 2048], P('dp', 'tp'), may hold values from -4 to 4
- q_rope: bfloat16 [4096, 1024], P('dp', 'tp'), may hold values from -80 to 80
- lengths: int32 [4096], P('dp'), may hold values from 1 to 512, as said below
- page_table: int32 [4096, 8], P('dp'), may hold values from 0 to 95, as said below
- lend_counts: int32 [4096, 2], P('dp'), may hold values from 0 to 2, as said below
- latent_pages: bfloat16 [12288, 64, 512], P('dp'), may hold values from -5 to 5
- rope_pages: bfloat16 [12288, 4096], P('dp'), may hold values from -4 to 4
- w_uk: bfloat16 [16, 128, 512], P('tp'), may hold values from -0.5 to 0.5
- w_uv: bfloat16 [16, 512, 128], P('tp'), may hold values from -0.75 to 0.75
- w_o: bfloat16 [2048, 2048], P('tp'), may hold values from -0.125 to 0.125
Outputs:
- attention_out: bfloat16 [4096, 2048], P('dp', 'tp')
The draws below stay inside these ranges and needn't reach their ends.
Inputs may be any that keep to these rules, and one draw needn't show every extreme that they name: `lengths`: at least one live token in every request; some request reaches the most in every draw. For every request lend_counts[r, 0] + lend_counts[r, 1] is below its page count, so its first page is held by its own replica; every replica has a request that lends 2 pages each way. `page_table`: the 8 entries of a row are distinct. Entries for pages past a request's page count are not read.
All inputs are finite; a program needn't handle non-finite values.
Results may differ from the reference program's by a relative error of at most 0.012.
Values may be sent and summed in bfloat16 or wider, within the bound.
A program may use at most 128 MiB of HBM per device.

```python
import math
import jax
import jax.numpy as jnp
from jax import lax

D = 2048
HEADS = 16
LATENT = 512
ROPE = 64
NOPE = 128
VDIM = 128
PAGE = 64
MAXP = 8
LEND = 2
REQS = 32
PAGES_DEV = 96
REQS_ALL = 4096
PAGES_ALL = 12288
N_DP = 128


def lend_plan(key):
    base_key = jax.random.fold_in(key, 11)
    key_busy, key_long, key_short, key_chosen, key_left, key_right, key_lender, key_full = jax.random.split(base_key, 8)
    replicas = REQS_ALL // REQS
    busy_replica = jax.random.randint(key_busy, (replicas,), 0, 4) == 0
    busy_rows = jnp.repeat(busy_replica, REQS)
    top_len = MAXP * PAGE
    long_len = jax.random.randint(key_long, (REQS_ALL,), top_len // 2, top_len + 1)
    short_len = jax.random.randint(key_short, (REQS_ALL,), 1, top_len // 4 + 1)
    req_lens = jnp.where(busy_rows, long_len, short_len)
    row_ids = jnp.arange(REQS_ALL, dtype=jnp.int32)
    lender_slot = jax.random.randint(key_lender, (replicas,), 0, REQS)
    lender_rows = jnp.arange(replicas, dtype=jnp.int32) * REQS + lender_slot
    is_lender = jnp.any(row_ids[:, None] == lender_rows[None, :], axis=1)
    full_len = jax.random.randint(key_full, (REQS_ALL,), (MAXP - 1) * PAGE + 1, top_len + 1)
    req_lens = jnp.where(is_lender, full_len, req_lens)
    chosen = jax.random.randint(key_chosen, (), 0, REQS_ALL)
    req_lens = jnp.where(row_ids == chosen, top_len, req_lens)
    page_count = (req_lens + PAGE - 1) // PAGE
    lend_left = jnp.minimum(jax.random.randint(key_left, (REQS_ALL,), 0, LEND + 1), (page_count - 1) // 2)
    lend_right = jnp.minimum(jax.random.randint(key_right, (REQS_ALL,), 0, LEND + 1), page_count - 1 - lend_left)
    forced = is_lender | (row_ids == chosen)
    lend_left = jnp.where(forced, LEND, lend_left)
    lend_right = jnp.where(forced, LEND, lend_right)
    return (req_lens.astype(jnp.int32), jnp.stack([lend_left, lend_right], axis=1).astype(jnp.int32))


def draw_lengths(key, part):
    return lend_plan(key)[0]


def draw_lend_counts(key, part):
    return lend_plan(key)[1]


def draw_page_table(key, part):
    row_keys = jax.random.split(jax.random.fold_in(key, 41), REQS_ALL)
    picked = jax.vmap(lambda one: jax.random.permutation(one, PAGES_DEV)[:MAXP])(row_keys)
    return picked.astype(jnp.int32)


def draw_q_rope(key, part):
    key_noise = jax.random.fold_in(jax.random.fold_in(key, 23), 0)
    values = jax.random.truncated_normal(key_noise, -4.0, 4.0, (REQS_ALL, HEADS, ROPE), jnp.float32)
    return values.reshape(REQS_ALL, HEADS * ROPE).astype(jnp.bfloat16)


def draw_rope_pages(key, part):
    key_noise = jax.random.fold_in(jax.random.fold_in(key, 31), 0)
    values = jax.random.truncated_normal(key_noise, -4.0, 4.0, (PAGES_ALL, PAGE, ROPE), jnp.float32)
    return values.reshape(PAGES_ALL, PAGE * ROPE).astype(jnp.bfloat16)


def steps_of(stream_key, extent, pieces, smallest, largest):
    factor_of, own = 1.0, jax.random.fold_in(stream_key, 6)
    for dim, blocks in pieces:
        steps = jnp.exp(jax.random.uniform(jax.random.fold_in(own, dim), (blocks,), jnp.float32, smallest / len(pieces), largest / len(pieces)))
        factor_of = factor_of * jnp.repeat(steps, extent[dim] // blocks).reshape([-1 if axis == dim else 1 for axis in range(len(extent))])
    return factor_of


def scatter_about(stream_key, shape, width, limit, pieces=(), kind=jnp.bfloat16):
    gain = steps_of(stream_key, shape, pieces, -0.22, 0.18) if pieces else 1.0
    array = jax.random.normal(stream_key, shape, jnp.float32) * width * gain
    return jnp.minimum(jnp.maximum(array, -limit), limit).astype(kind)


def setup_inputs(seed: int = 0) -> dict:
    splits = jax.random.split(jax.random.key(seed), 11)
    return {
        "q_nope": scatter_about(splits[0], (REQS_ALL, HEADS * NOPE), 1.0, 4.0, ((0, 128), (1, 2))),
        "q_rope": draw_q_rope(jax.random.fold_in(splits[10], 71), 0),
        "lengths": draw_lengths(jax.random.fold_in(splits[10], 71), 0),
        "page_table": draw_page_table(jax.random.fold_in(splits[10], 71), 0),
        "lend_counts": draw_lend_counts(jax.random.fold_in(splits[10], 71), 0),
        "latent_pages": scatter_about(splits[5], (PAGES_ALL, PAGE, LATENT), 1.0, 5.0, ((0, 128),)),
        "rope_pages": draw_rope_pages(jax.random.fold_in(splits[10], 71), 0),
        "w_uk": scatter_about(splits[7], (HEADS, NOPE, LATENT), NOPE ** -0.5, 0.5, ((0, 2),)),
        "w_uv": scatter_about(splits[8], (HEADS, LATENT, VDIM), (LATENT // 8) ** -0.5, 0.75, ((0, 2),)),
        "w_o": scatter_about(splits[9], (HEADS * VDIM, D), (HEADS * VDIM) ** -0.5, 0.125, ((0, 2),)),
    }


def reference(q_nope, q_rope, lengths, page_table, lend_counts, latent_pages, rope_pages, w_uk, w_uv, w_o):
    score_scale = 1.0 / math.sqrt(NOPE + ROPE)
    query_lat = jnp.einsum('rhn,hnc->rhc', q_nope.reshape(REQS_ALL, HEADS, NOPE).astype(jnp.float32), w_uk.astype(jnp.float32)).astype(jnp.bfloat16)
    query_rope = q_rope.reshape(REQS_ALL, HEADS, ROPE)
    rope_table = rope_pages.reshape(PAGES_ALL, PAGE, ROPE)

    def replica(index):
        row_start = (index * REQS).astype(jnp.int32)
        req_lens = lax.dynamic_slice_in_dim(lengths, row_start, REQS)
        slot_table = lax.dynamic_slice_in_dim(page_table, row_start, REQS)
        lend_rows = lax.dynamic_slice_in_dim(lend_counts, row_start, REQS)
        own_query = lax.dynamic_slice_in_dim(query_lat, row_start, REQS)
        own_rope = lax.dynamic_slice_in_dim(query_rope, row_start, REQS)
        page_count = (req_lens + PAGE - 1) // PAGE
        first_lent = (page_count - lend_rows[:, 0] - lend_rows[:, 1])[:, None]
        second = (page_count - lend_rows[:, 1])[:, None]
        page_ids = jnp.arange(MAXP, dtype=jnp.int32)[None, :]
        holder_step = jnp.where(page_ids < first_lent, 0, jnp.where(page_ids < second, N_DP - 1, 1)).astype(jnp.int32)
        holder = (index + holder_step) % N_DP
        pool_rows = (holder * PAGES_DEV + slot_table).astype(jnp.int32)
        latent = latent_pages[pool_rows].reshape(REQS, MAXP * PAGE, LATENT).astype(jnp.float32)
        rope_keys = rope_table[pool_rows].reshape(REQS, MAXP * PAGE, ROPE).astype(jnp.float32)
        positions = jnp.arange(MAXP * PAGE, dtype=jnp.int32)[None, :]
        alive_mask = positions < req_lens[:, None]
        scores = (jnp.einsum('rhc,rtc->rht', own_query.astype(jnp.float32), latent) + jnp.einsum('rhe,rte->rht', own_rope.astype(jnp.float32), rope_keys)) * score_scale
        scores = jnp.where(alive_mask[:, None, :], scores, -jnp.inf)
        peak = lax.optimization_barrier(jnp.max(scores, axis=-1, keepdims=True))
        weights = jnp.exp(scores - peak).astype(jnp.bfloat16).astype(jnp.float32)
        total = lax.optimization_barrier(jnp.sum(weights, axis=-1))
        context = jnp.einsum('rht,rtc->rhc', weights, latent) / total[..., None]
        return context.astype(jnp.bfloat16)
    contexts = lax.map(replica, jnp.arange(N_DP, dtype=jnp.int32)).reshape(REQS_ALL, HEADS, LATENT)
    head_outs = jnp.einsum('rhc,hcv->rhv', contexts.astype(jnp.float32), w_uv.astype(jnp.float32)).astype(jnp.bfloat16)
    head_outs = head_outs.reshape(REQS_ALL, HEADS * VDIM)
    return jnp.dot(head_outs, w_o, preferred_element_type=jnp.float32).astype(jnp.bfloat16)
```

```python
import functools
import math

import jax
import jax.numpy as jnp
from jax import lax
from jax.experimental import pallas as pl
from jax.experimental.pallas import tpu as pltpu
from jax.sharding import PartitionSpec as P

ROPE = 64
NOPE = 128
VDIM = 128
PAGE = 64
MAXP = 8
LEND = 2
MESH = pl.DeviceIdType.MESH
NEG = -3e38
SCALE2 = math.log2(math.e) / math.sqrt(NOPE + ROPE)
COL_A, COL_B, COL_LEN = 8, 9, 10
CHUNK_PAGES = 16
F32 = jnp.float32
BF16 = jnp.bfloat16


def dot(a, b):
    return lax.dot_general(a, b, (((1,), (0,)), ((), ())), preferred_element_type=F32)


def dot_t(a, b):
    return lax.dot_general(a, b, (((1,), (1,)), ((), ())), preferred_element_type=F32)


def iota(shape, dim):
    return lax.broadcasted_iota(jnp.int32, shape, dim)


def doubled_rope(q_rope, head):
    pair = q_rope[:, (head // 2) * 128 : (head // 2 + 1) * 128].astype(F32)
    turned = pltpu.roll(pair, 64, 1)
    low = iota(pair.shape, 1) < 64
    return jnp.where(low, pair, turned) if head % 2 == 0 else jnp.where(low, turned, pair)


def kernel(
    n_dp,
    qn_hbm, qr_hbm, tab_hbm, lat_hbm, rope_hbm, wuk_hbm, wuv_hbm, wo_hbm,
    out_ref,
    qn, qr, tab, plan, lat, rope, wuk, wuv, wo,
    qn_in, qr_in, tab_in, tab_sm,
    perm, keys, q_own, bias, scores, probs, acc,
    q_far, s_far, o_far, m_far, l_far,
    u_out, ml_out, u_in, ml_in, heads_out, y_out, y_in,
    load_sem, lat_sem, sm_sem, qsend_sem, qrecv_sem, usend_sem, urecv_sem, ysend_sem, yrecv_sem,
):
    reqs = qn.shape[0]
    n_heads = wuk.shape[0]
    slots = rope.shape[0]
    latent = lat.shape[2]
    half = wo.shape[2]
    rows = reqs * n_heads
    chunk = CHUNK_PAGES * PAGE

    me = lax.axis_index("dp")
    side = lax.axis_index("tp")
    nxt = lax.rem(me + 1, n_dp)
    prv = lax.rem(me + n_dp - 1, n_dp)

    def local(src, dst, i):
        copy = pltpu.make_async_copy(src, dst, load_sem.at[i])
        copy.start()
        return copy

    c_qn = local(qn_hbm, qn, 0)
    c_qr = local(qr_hbm, qr, 1)
    c_tab = local(tab_hbm, tab, 2)
    c_wuk = local(wuk_hbm, wuk, 3)
    c_rope = local(rope_hbm, rope, 4)
    c_lat = []
    for i in range(slots // CHUNK_PAGES):
        part = pl.ds(i * CHUNK_PAGES, CHUNK_PAGES)
        copy = pltpu.make_async_copy(lat_hbm.at[part], lat.at[part], lat_sem.at[i])
        copy.start()
        c_lat.append(copy)
    c_wuv = local(wuv_hbm, wuv, 5)
    c_wo0 = local(wo_hbm.at[:, pl.ds((1 - side) * half, half)], wo.at[0], 6)
    c_wo1 = local(wo_hbm.at[:, pl.ds(side * half, half)], wo.at[1], 7)

    barrier = pltpu.get_barrier_semaphore()
    pl.semaphore_signal(barrier, inc=1, device_id={"dp": prv}, device_id_type=MESH)
    pl.semaphore_signal(barrier, inc=1, device_id={"dp": nxt}, device_id_type=MESH)
    pl.semaphore_signal(barrier, inc=1, device_id={"tp": 1 - side}, device_id_type=MESH)
    pl.semaphore_wait(barrier, 3)

    def ask(d, i, src, dst):
        copy = pltpu.make_async_remote_copy(
            src_ref=src, dst_ref=dst.at[d],
            send_sem=qsend_sem.at[d, i], recv_sem=qrecv_sem.at[d, i],
            device_id={"dp": prv if d == 0 else nxt}, device_id_type=MESH,
        )
        copy.start()
        return copy

    c_qn.wait()
    c_qr.wait()
    asks = [[ask(d, 0, qn, qn_in), ask(d, 1, qr, qr_in)] for d in range(2)]
    c_tab.wait()

    lane = iota((reqs, 128), 1)

    def column(i):
        return jnp.broadcast_to(tab[:, i : i + 1], (reqs, 128))

    table = [column(k) for k in range(MAXP)]
    length = column(COL_LEN)
    n_pages = (length + (PAGE - 1)) >> 6
    first = n_pages - column(COL_A) - column(COL_B)
    for d in range(2):
        start = first if d == 0 else n_pages - column(COL_B)
        held = column(COL_A + d)
        packed = jnp.zeros((reqs, 128), jnp.int32)
        for j in range(LEND):
            at = start + j
            slot = jnp.zeros((reqs, 128), jnp.int32)
            for k in range(MAXP):
                slot = jnp.where(at == k, table[k], slot)
            used = held > j
            slot = jnp.where(used, jnp.clip(slot, 0, slots - 1), 0)
            live = jnp.where(used, jnp.clip(length - at * PAGE, 0, PAGE), 0)
            packed = jnp.where(lane == j, slot, packed)
            packed = jnp.where(lane == LEND + j, live, packed)
        plan[d] = packed
    for d in range(2):
        asks[d].append(ask(d, 2, plan.at[d], tab_in))

    out_row = iota((512, 256), 0)
    in_row = iota((512, 256), 1)
    hit = ((out_row >> 5) == (in_row & 15)) & (((out_row & 31) >> 1) == (in_row >> 4))
    perm[...] = jnp.where(hit, 1.0, 0.0).astype(BF16)

    count = jnp.zeros((reqs, 128), jnp.int32)
    for k in range(MAXP):
        live = jnp.clip(length - k * PAGE, 0, PAGE)
        count = count + jnp.where((lane == table[k]) & (first > k), live, 0)
    for g in range(slots // 2):
        even = jnp.broadcast_to(count[:, 2 * g : 2 * g + 1], (reqs, 128))
        odd = jnp.broadcast_to(count[:, 2 * g + 1 : 2 * g + 2], (reqs, 128))
        limit = jnp.where(lane < 64, even, odd)
        bias[:, g * 128 : (g + 1) * 128] = jnp.where((lane & 63) < limit, 0.0, NEG)

    c_wuk.wait()
    for h in range(n_heads):
        mine = pl.ds(h * reqs, reqs)
        q_own[mine, 0:latent] = dot(qn[:, h * NOPE : (h + 1) * NOPE], wuk[h]).astype(BF16)
        q_own[mine, latent : latent + 128] = doubled_rope(qr, h).astype(BF16)

    c_rope.wait()
    row_odd = (iota((512, 128), 0) & 1) == 1
    lane_high = iota((512, 128), 1) >= 64
    keep = row_odd == lane_high
    for g in range(slots // 16):
        page_rows = pl.ds(g * 16, 16)
        left = jnp.concatenate(
            [rope[page_rows, j * 128 : (j + 1) * 128] for j in range(16)], axis=0
        )
        right = jnp.concatenate(
            [rope[page_rows, (16 + j) * 128 : (17 + j) * 128] for j in range(16)], axis=0
        )
        moved = dot(perm[...], jnp.concatenate([left, right], axis=1))
        for s in range(2):
            part = jnp.where(keep, moved[:, s * 128 : (s + 1) * 128], 0.0).astype(BF16)
            keys[page_rows, s * 32 : (s + 1) * 32, :] = part.reshape(16, 32, 128)

    top = None
    for i in range(slots // CHUNK_PAGES):
        c_lat[i].wait()
        for j in range(CHUNK_PAGES // 4):
            page0 = i * CHUNK_PAGES + j * 4
            at = page0 * PAGE
            s = dot_t(q_own[:, 0:latent], lat[page0 : page0 + 4].reshape(256, latent))
            s = s + dot_t(
                q_own[:, latent : latent + 128], keys[page0 : page0 + 4].reshape(256, 128)
            )
            b = bias[:, at : at + 256]
            s = (s.reshape(n_heads, reqs, 256) + b[None]).reshape(rows, 256)
            scores[:, at : at + 256] = s
            peak = jnp.maximum(s[:, 0:128], s[:, 128:256])
            top = peak if top is None else jnp.maximum(top, peak)
    top = jnp.max(top, axis=1, keepdims=True)

    for d in range(2):
        asks[d][2].wait_recv()
    c_sm = pltpu.make_async_copy(tab_in, tab_sm, sm_sem)
    c_sm.start()
    for d in range(2):
        asks[d][0].wait_recv()
        asks[d][1].wait_recv()
    for d in range(2):
        for h in range(n_heads):
            far = dot(qn_in[d, :, h * NOPE : (h + 1) * NOPE], wuk[h])
            at = pl.ds(d * n_heads + h, reqs, stride=2 * n_heads)
            for j in range(latent // 128):
                q_far[j, at, :] = far[:, j * 128 : (j + 1) * 128]
            q_far[latent // 128, at, :] = doubled_rope(qr_in.at[d], h)
    c_sm.wait()

    def pages_of(r):
        found = []
        for d in range(2):
            for j in range(LEND):
                found.append((tab_sm[d, r, j], tab_sm[d, r, LEND + j]))
        return found

    lane8 = iota((8, 128), 1)

    def far_scores(step, carry):
        for u in range(4):
            r = step * 4 + u
            found = pages_of(r)
            at = pl.ds(pl.multiple_of(r * 16, 16), 16)
            k_lat = jnp.concatenate(
                [lat[slot] for slot, _ in found], axis=0
            )
            k_rope = jnp.concatenate([keys[slot] for slot, _ in found], axis=0)
            q_lat = jnp.concatenate(
                [q_far[j, at, :] for j in range(latent // 128)], axis=1
            ).astype(BF16)
            s = dot_t(q_lat, k_lat) + dot_t(q_far[latent // 128, at, :].astype(BF16), k_rope)
            for d in range(2):
                limit = jnp.where(lane8 < 64, found[2 * d][1], found[2 * d + 1][1])
                part = s[d * 8 : (d + 1) * 8, d * 128 : (d + 1) * 128]
                part = jnp.where((lane8 & 63) < limit, part, NEG)
                s_far[pl.ds(pl.multiple_of(r * 16 + d * 8, 8), 8), :] = part
        return carry

    lax.fori_loop(0, reqs // 4, far_scores, 0)

    s = s_far[...]
    peak = jnp.maximum(jnp.max(s, axis=1, keepdims=True), -1e30)
    w = jnp.exp2((s - peak) * SCALE2)
    m_far[...] = jnp.broadcast_to(peak, s.shape)
    l_far[...] = jnp.broadcast_to(jnp.sum(w, axis=1, keepdims=True), s.shape)
    s_far[...] = w

    first_half = iota((16, 128), 0) < 8

    def far_values(step, carry):
        for u in range(4):
            r = step * 4 + u
            found = pages_of(r)
            at = pl.ds(pl.multiple_of(r * 16, 16), 16)
            w = s_far[at, :]
            w = jnp.concatenate(
                [jnp.where(first_half, w, 0.0), jnp.where(first_half, 0.0, w)], axis=1
            ).astype(BF16)
            v = jnp.concatenate(
                [lat[slot] for slot, _ in found], axis=0
            )
            o = dot(w, v)
            for j in range(latent // 128):
                o_far[j, at, :] = o[:, j * 128 : (j + 1) * 128]
        return carry

    lax.fori_loop(0, reqs // 4, far_values, 0)

    c_wuv.wait()
    packs = [jnp.zeros((reqs, 128), F32) for _ in range(2)]
    for h in range(n_heads):
        o = []
        for d in range(2):
            at = pl.ds(d * n_heads + h, reqs, stride=2 * n_heads)
            o.append(
                jnp.concatenate([o_far[j, at, :] for j in range(latent // 128)], axis=1)
            )
            packs[d] = jnp.where(lane == h, m_far[at, :], packs[d])
            packs[d] = jnp.where(lane == n_heads + h, l_far[at, :], packs[d])
        u = dot(jnp.concatenate(o, axis=0).astype(BF16), wuv[h]).astype(BF16)
        for d in range(2):
            u_out[d, :, h * VDIM : (h + 1) * VDIM] = u[d * reqs : (d + 1) * reqs]
    for d in range(2):
        ml_out[d] = packs[d]

    backs = []
    for d, target in ((0, nxt), (1, prv)):
        duo = []
        for i, (src, dst) in enumerate(((ml_out, ml_in), (u_out, u_in))):
            copy = pltpu.make_async_remote_copy(
                src_ref=src.at[d], dst_ref=dst.at[d],
                send_sem=usend_sem.at[d, i], recv_sem=urecv_sem.at[d, i],
                device_id={"dp": target}, device_id_type=MESH,
            )
            copy.start()
            duo.append(copy)
        backs.append(duo)

    total = jnp.zeros((rows, 128), F32)
    for i in range(slots // CHUNK_PAGES):
        for j in range(CHUNK_PAGES // 2):
            at = i * chunk + j * 128
            w = jnp.exp2((scores[:, at : at + 128] - top) * SCALE2)
            total = total + w
            probs[:, at : at + 128] = w.astype(BF16)
        part = dot(probs[:, i * chunk : (i + 1) * chunk], lat[i * CHUNK_PAGES : (i + 1) * CHUNK_PAGES].reshape(chunk, latent))
        if i == 0:
            acc[...] = part
        else:
            acc[...] += part
    total = jnp.sum(total, axis=1, keepdims=True)

    own_u = []
    for h in range(n_heads):
        own_u.append(dot(acc[h * reqs : (h + 1) * reqs, :].astype(BF16), wuv[h]))

    for d in range(2):
        for copy in backs[d]:
            copy.wait_recv()
    for h in range(n_heads):
        mine = slice(h * reqs, (h + 1) * reqs)
        ms = [top[mine]] + [ml_in[d, :, h : h + 1] for d in range(2)]
        ls = [total[mine]] + [ml_in[d, :, n_heads + h : n_heads + h + 1] for d in range(2)]
        us = [own_u[h]] + [
            u_in[d, :, h * VDIM : (h + 1) * VDIM].astype(F32) for d in range(2)
        ]
        peak = jnp.maximum(jnp.maximum(ms[0], ms[1]), ms[2])
        fs = [jnp.exp2((m - peak) * SCALE2) for m in ms]
        den = fs[0] * ls[0] + fs[1] * ls[1] + fs[2] * ls[2]
        num = fs[0] * us[0] + fs[1] * us[1] + fs[2] * us[2]
        heads_out[:, h * VDIM : (h + 1) * VDIM] = (num / den).astype(BF16)

    c_wo0.wait()
    c_wo1.wait()
    y_out[...] = dot(heads_out[...], wo[0]).astype(BF16)
    c_y = pltpu.make_async_remote_copy(
        src_ref=y_out, dst_ref=y_in, send_sem=ysend_sem, recv_sem=yrecv_sem,
        device_id={"tp": 1 - side}, device_id_type=MESH,
    )
    c_y.start()
    mine = dot(heads_out[...], wo[1])
    c_y.wait()
    out_ref[...] = (mine + y_in[...].astype(F32)).astype(BF16)
    for d in range(2):
        for copy in asks[d]:
            copy.wait_send()
        for copy in backs[d]:
            copy.wait_send()


def shards(
    n_dp, q_nope, q_rope, lengths, page_table, lend_counts, latent_pages, rope_pages, w_uk, w_uv, w_o
):
    reqs = lengths.shape[0]
    slots, _, latent = latent_pages.shape
    n_heads = w_uk.shape[0]
    half = w_o.shape[1] // 2
    rows = reqs * n_heads
    tokens = slots * PAGE
    tab = jnp.concatenate(
        [page_table, lend_counts, lengths[:, None], jnp.zeros((reqs, 117), jnp.int32)], axis=1
    )
    vmem = pltpu.VMEM
    dma = pltpu.SemaphoreType.DMA
    n_chunks = slots // CHUNK_PAGES
    return pl.pallas_call(
        functools.partial(kernel, n_dp),
        out_shape=jax.ShapeDtypeStruct((reqs, half), BF16),
        in_specs=[pl.BlockSpec(memory_space=pl.ANY)] * 8,
        out_specs=pl.BlockSpec(memory_space=vmem),
        scratch_shapes=[
            vmem(q_nope.shape, BF16),
            vmem(q_rope.shape, BF16),
            vmem((reqs, 128), jnp.int32),
            vmem((2, reqs, 128), jnp.int32),
            vmem((slots, PAGE, latent), BF16),
            vmem(rope_pages.shape, BF16),
            vmem(w_uk.shape, BF16),
            vmem(w_uv.shape, BF16),
            vmem((2, w_o.shape[0], half), BF16),
            vmem((2, *q_nope.shape), BF16),
            vmem((2, *q_rope.shape), BF16),
            vmem((2, reqs, 128), jnp.int32),
            pltpu.SMEM((2, reqs, 128), jnp.int32),
            vmem((512, 256), BF16),
            vmem((slots, PAGE, 128), BF16),
            vmem((rows, latent + 128), BF16),
            vmem((reqs, tokens), F32),
            vmem((rows, tokens), F32),
            vmem((rows, tokens), BF16),
            vmem((rows, latent), F32),
            vmem((latent // 128 + 1, 2 * rows, 128), F32),
            vmem((2 * rows, 128), F32),
            vmem((latent // 128, 2 * rows, 128), F32),
            vmem((2 * rows, 128), F32),
            vmem((2 * rows, 128), F32),
            vmem((2, reqs, n_heads * VDIM), BF16),
            vmem((2, reqs, 128), F32),
            vmem((2, reqs, n_heads * VDIM), BF16),
            vmem((2, reqs, 128), F32),
            vmem((reqs, n_heads * VDIM), BF16),
            vmem((reqs, half), BF16),
            vmem((reqs, half), BF16),
            dma((8,)),
            dma((n_chunks,)),
            dma,
            dma((2, 3)),
            dma((2, 3)),
            dma((2, 2)),
            dma((2, 2)),
            dma,
            dma,
        ],
        compiler_params=pltpu.CompilerParams(
            collective_id=0, has_side_effects=True, vmem_limit_bytes=60 * 1024 * 1024
        ),
        name="latent_step",
    )(
        q_nope, q_rope, tab, latent_pages, rope_pages, w_uk, w_uv, w_o
    )


def solution(mesh):
    in_specs = (
        P("dp", "tp"),
        P("dp", "tp"),
        P("dp"),
        P("dp", None),
        P("dp", None),
        P("dp", None, None),
        P("dp", None),
        P("tp", None, None),
        P("tp", None, None),
        P("tp", None),
    )
    return jax.shard_map(
        functools.partial(shards, mesh.shape["dp"]),
        mesh=mesh, in_specs=in_specs, out_specs=P("dp", "tp"), check_vma=False,
    )
```

```python
import functools
import math

import jax
import jax.numpy as jnp
from jax import lax
from jax.experimental import pallas as pl
from jax.experimental.pallas import tpu as pltpu
from jax.sharding import PartitionSpec as P

ROPE = 64
NOPE = 128
VDIM = 128
PAGE = 64
MAXP = 8
LEND = 2
MESH = pl.DeviceIdType.MESH
NEG = -3e38
SCALE2 = math.log2(math.e) / math.sqrt(NOPE + ROPE)
GROUP = 4
PARTS = 2
F32 = jnp.float32
BF16 = jnp.bfloat16

def dot(a, b):
    return lax.dot_general(a, b, (((1,), (0,)), ((), ())), preferred_element_type=F32)

def dot_t(a, b):
    return lax.dot_general(a, b, (((1,), (1,)), ((), ())), preferred_element_type=F32)

def iota(shape, dim):
    return lax.broadcasted_iota(jnp.int32, shape, dim)

def doubled_rope(q_rope, head):
    pair = q_rope[:, (head // 2) * 128 : (head // 2 + 1) * 128].astype(F32)
    turned = pltpu.roll(pair, 64, 1)
    low = iota(pair.shape, 1) < 64
    return jnp.where(low, pair, turned) if head % 2 == 0 else jnp.where(low, turned, pair)

def kernel(
    n_dp,
    qn_hbm, qr_hbm, table_hbm, lent_hbm, size_hbm, lat_hbm, rope_hbm, wuk_hbm, wuv_hbm, wo_hbm,
    out_ref,
    qn, qr, table, lent, size, plan, lat, rope, wuk, wuv, wo,
    qn_in, qr_in, plan_in, plan_sm,
    perm, keys, q_own, bias, scores, peaks, probs, acc,
    q_far, o_far, m_far, l_far,
    u_out, ml_out, u_in, ml_in, heads_out, y_out, y_in,
    load_sem, sm_sem, qsend_sem, qrecv_sem, usend_sem, urecv_sem, ysend_sem, yrecv_sem,
):
    reqs = qn.shape[0]
    n_heads = wuk.shape[0]
    slots = rope.shape[0]
    latent = lat.shape[2]
    wide = latent // 128
    half = out_ref.shape[1]
    rows = reqs * n_heads
    parts = y_out.shape[0]
    piece = half // parts

    me = lax.axis_index("dp")
    side = lax.axis_index("tp")
    nxt = lax.rem(me + 1, n_dp)
    prv = lax.rem(me + n_dp - 1, n_dp)
    near = jnp.where(me == 1, 0, lax.rem(me, 2))

    def local(src, dst, i):
        copy = pltpu.make_async_copy(src, dst, load_sem.at[i])
        copy.start()
        return copy

    barrier = pltpu.get_barrier_semaphore()
    pl.semaphore_signal(barrier, inc=1, device_id={"dp": prv}, device_id_type=MESH)
    pl.semaphore_signal(barrier, inc=1, device_id={"dp": nxt}, device_id_type=MESH)
    pl.semaphore_signal(barrier, inc=1, device_id={"tp": 1 - side}, device_id_type=MESH)
    c_table = local(table_hbm, table, 0)
    c_lent = local(lent_hbm, lent, 1)
    c_size = local(size_hbm, size, 2)
    c_rope = local(rope_hbm, rope, 5)
    c_qn = local(qn_hbm, qn, 3)
    c_qr = local(qr_hbm, qr, 4)
    c_wuk = local(wuk_hbm, wuk, 6)
    thirds = slots // 3
    c_lat = [
        local(lat_hbm.at[pl.ds(i * thirds, thirds)], lat.at[pl.ds(i * thirds, thirds)], 7 + i)
        for i in range(3)
    ]

    out_row = iota((512, 256), 0)
    in_row = iota((512, 256), 1)
    hit = ((out_row >> 5) == (in_row & 15)) & (((out_row & 31) >> 1) == (in_row >> 4))
    perm[...] = jnp.where(hit, 1.0, 0.0).astype(BF16)

    c_table.wait()
    c_lent.wait()
    c_size.wait()

    def spread(row):
        return jnp.broadcast_to(row, (8, reqs))

    row8 = iota((8, reqs), 0)
    pages = table[...]
    length = spread(size[...])
    lent_left = spread(lent[0:1, :])
    lent_right = spread(lent[1:2, :])
    n_pages = (length + (PAGE - 1)) >> 6
    first = n_pages - lent_left - lent_right
    for d in range(2):
        start = first if d == 0 else n_pages - lent_right
        held = lent_left if d == 0 else lent_right
        packed = jnp.zeros((8, reqs), jnp.int32)
        for j in range(LEND):
            at = start + j
            slot = spread(jnp.sum(jnp.where(row8 == at, pages, 0), axis=0, keepdims=True))
            used = held > j
            slot = jnp.where(used, jnp.clip(slot, 0, slots - 1), 0)
            live = jnp.where(used, jnp.clip(length - at * PAGE, 0, PAGE), 0)
            packed = jnp.where(row8 == j, slot, packed)
            packed = jnp.where(row8 == LEND + j, live, packed)
        plan[d, :, 0:reqs] = packed

    lane = iota((reqs, 128), 1)
    facts = jnp.concatenate([pages, first, length], axis=0).astype(F32)
    facts = jnp.concatenate([facts, jnp.zeros((24, 128 - reqs), F32)], axis=1)
    facts = jnp.concatenate([facts, jnp.zeros((104, 128), F32)], axis=0)
    facts = jnp.transpose(facts)[0:reqs].astype(jnp.int32)

    def column(i):
        return jnp.broadcast_to(facts[:, i : i + 1], (reqs, 128))

    first = column(8)
    length = column(16)
    count = jnp.zeros((reqs, 128), jnp.int32)
    for k in range(MAXP):
        live = jnp.clip(length - k * PAGE, 0, PAGE)
        count = count + jnp.where((lane == column(k)) & (first > k), live, 0)
    for g in range(slots // 2):
        even = jnp.broadcast_to(count[:, 2 * g : 2 * g + 1], (reqs, 128))
        odd = jnp.broadcast_to(count[:, 2 * g + 1 : 2 * g + 2], (reqs, 128))
        limit = jnp.where(lane < 64, even, odd)
        bias[:, g * 128 : (g + 1) * 128] = jnp.where((lane & 63) < limit, 0.0, NEG)

    c_rope.wait()
    row_odd = (iota((512, 128), 0) & 1) == 1
    lane_high = iota((512, 128), 1) >= 64
    keep = row_odd == lane_high
    for g in range(slots // 16):
        page_rows = pl.ds(g * 16, 16)
        left = jnp.concatenate(
            [rope[page_rows, j * 128 : (j + 1) * 128] for j in range(16)], axis=0
        )
        right = jnp.concatenate(
            [rope[page_rows, (16 + j) * 128 : (17 + j) * 128] for j in range(16)], axis=0
        )
        moved = dot(perm[...], jnp.concatenate([left, right], axis=1))
        for s in range(2):
            part = jnp.where(keep, moved[:, s * 128 : (s + 1) * 128], 0.0).astype(BF16)
            keys[page_rows, s * 32 : (s + 1) * 32, :] = part.reshape(16, 32, 128)

    c_qn.wait()
    c_qr.wait()

    def pool_ready():
        c_wuk.wait()
        for copy in c_lat:
            copy.wait()

    def own_scores():
        for h in range(n_heads):
            mine = pl.ds(h * reqs, reqs)
            q_own[mine, 0:latent] = dot(qn[:, h * NOPE : (h + 1) * NOPE], wuk[h]).astype(BF16)
            q_own[mine, latent : latent + 128] = doubled_rope(qr, h).astype(BF16)
        top = None
        for i in range(slots // 4):
            at = i * 4 * PAGE
            s = dot_t(q_own[:, 0:latent], lat[i * 4 : i * 4 + 4].reshape(256, latent))
            s = s + dot_t(
                q_own[:, latent : latent + 128], keys[i * 4 : i * 4 + 4].reshape(256, 128)
            )
            b = bias[:, at : at + 256]
            s = (s.reshape(n_heads, reqs, 256) + b[None]).reshape(rows, 256)
            scores[:, at : at + 256] = s
            peak = jnp.maximum(s[:, 0:128], s[:, 128:256])
            top = peak if top is None else jnp.maximum(top, peak)
        peaks[...] = top

    def early_scores():
        pool_ready()
        own_scores()

    pl.when(me <= 1)(early_scores)

    pl.semaphore_wait(barrier, 3)

    def ask(d, i, src, dst):
        return pltpu.make_async_remote_copy(
            src_ref=src, dst_ref=dst.at[d],
            send_sem=qsend_sem.at[d, i], recv_sem=qrecv_sem.at[d, i],
            device_id={"dp": prv if isinstance(d, int) and d == 0 else nxt}, device_id_type=MESH,
        )

    asks = []
    for d in range(2):
        asks.append(ask(d, 2, plan.at[d], plan_in))
        asks.append(ask(d, 0, qn, qn_in))
        asks.append(ask(d, 1, qr, qr_in))
    for copy in asks:
        copy.start()
    c_wuv = local(wuv_hbm, wuv, 10)
    c_wo = [
        local(
            wo_hbm.at[:, pl.ds((1 - side) * half + p * piece, piece)], wo.at[p], 11 + p
        )
        for p in range(parts)
    ] + [
        local(wo_hbm.at[:, pl.ds(side * half + p * piece, piece)], wo.at[parts + p], 11 + parts + p)
        for p in range(parts)
    ]

    pl.when(me > 1)(pool_ready)
    lane8 = iota((8, 128), 1)

    def far_terms(d, wuv_copy):
        ask(d, 2, plan.at[0], plan_in).wait_recv()
        c_sm = pltpu.make_async_copy(plan_in.at[d], plan_sm.at[d], sm_sem.at[d])
        c_sm.start()
        ask(d, 0, qn, qn_in).wait_recv()
        ask(d, 1, qr, qr_in).wait_recv()
        q_rope = qr_in[d]
        for h in range(n_heads):
            far = dot(qn_in[d, :, h * NOPE : (h + 1) * NOPE], wuk[h])
            at = pl.ds(h, reqs, stride=n_heads)
            for j in range(wide):
                q_far[j, at, :] = far[:, j * 128 : (j + 1) * 128]
            q_far[wide, at, :] = doubled_rope(q_rope, h)
        c_sm.wait()

        def held(pair):
            return [
                (plan_sm[d, j, r], plan_sm[d, LEND + j, r])
                for r in (2 * pair, 2 * pair + 1)
                for j in range(LEND)
            ]

        def far_weights(pair):
            found = held(pair)
            at = slice(pair * 16, pair * 16 + 16)
            k_lat = jnp.concatenate([lat[slot] for slot, _ in found], axis=0)
            k_rope = jnp.concatenate([keys[slot] for slot, _ in found], axis=0)
            q_lat = jnp.concatenate([q_far[j, at, :] for j in range(wide)], axis=1).astype(BF16)
            s = dot_t(q_lat, k_lat) + dot_t(q_far[wide, at, :].astype(BF16), k_rope)
            blocks = []
            for e in range(2):
                limit = jnp.where(lane8 < 64, found[2 * e][1], found[2 * e + 1][1])
                part = s[e * 8 : (e + 1) * 8, e * 128 : (e + 1) * 128]
                part = jnp.where((lane8 & 63) < limit, part, NEG)
                peak = jnp.maximum(jnp.max(part, axis=1, keepdims=True), -1e30)
                w = jnp.exp2((part - peak) * SCALE2)
                total = jnp.sum(w, axis=1, keepdims=True)
                here = slice(pair * 16 + e * 8, pair * 16 + e * 8 + 8)
                m_far[here, :] = jnp.broadcast_to(peak, (8, 128))
                l_far[here, :] = jnp.broadcast_to(total, (8, 128))
                blocks.append(w)
            return blocks

        def far_values(pair, blocks):
            found = held(pair)
            none = jnp.zeros((8, 128), F32)
            w = jnp.concatenate(
                [
                    jnp.concatenate([blocks[0], none], axis=1),
                    jnp.concatenate([none, blocks[1]], axis=1),
                ],
                axis=0,
            ).astype(BF16)
            o = dot(w, jnp.concatenate([lat[slot] for slot, _ in found], axis=0))
            for j in range(wide):
                o_far[j, pair * 16 : pair * 16 + 16, :] = o[:, j * 128 : (j + 1) * 128]

        pairs = reqs // 2
        waiting = {}
        for pair in range(pairs + GROUP):
            if pair < pairs:
                waiting[pair] = far_weights(pair)
            if pair >= GROUP:
                far_values(pair - GROUP, waiting.pop(pair - GROUP))

        if wuv_copy is not None:
            wuv_copy.wait()
        pack = jnp.zeros((reqs, 128), F32)
        for h in range(n_heads):
            at = pl.ds(h, reqs, stride=n_heads)
            o = jnp.concatenate([o_far[j, at, :] for j in range(wide)], axis=1)
            u_out[d, :, h * VDIM : (h + 1) * VDIM] = dot(o.astype(BF16), wuv[h]).astype(BF16)
            pack = jnp.where(lane == h, m_far[at, :], pack)
            pack = jnp.where(lane == n_heads + h, l_far[at, :], pack)
        ml_out[d] = pack
        backs = []
        for i, (src, dst) in enumerate(((ml_out, ml_in), (u_out, u_in))):
            copy = pltpu.make_async_remote_copy(
                src_ref=src.at[d], dst_ref=dst.at[d],
                send_sem=usend_sem.at[d, i], recv_sem=urecv_sem.at[d, i],
                device_id={"dp": jnp.where(d == 0, nxt, prv)}, device_id_type=MESH,
            )
            copy.start()
            backs.append(copy)
        return backs

    backs = far_terms(near, c_wuv)

    backs += far_terms(1 - near, None)

    pl.when(me > 1)(own_scores)


    top = jnp.max(peaks[...], axis=1, keepdims=True)
    total = jnp.zeros((rows, 128), F32)
    span = 16 * PAGE
    for i in range(slots // 16):
        for j in range(span // 128):
            at = i * span + j * 128
            w = jnp.exp2((scores[:, at : at + 128] - top) * SCALE2)
            total = total + w
            probs[:, at : at + 128] = w.astype(BF16)
        part = dot(
            probs[:, i * span : (i + 1) * span], lat[i * 16 : (i + 1) * 16].reshape(span, latent)
        )
        if i == 0:
            acc[...] = part
        else:
            acc[...] += part
    total = jnp.sum(total, axis=1, keepdims=True)

    own_u = []
    m_own = jnp.zeros((reqs, 128), F32)
    l_own = jnp.zeros((reqs, 128), F32)
    for h in range(n_heads):
        mine = slice(h * reqs, (h + 1) * reqs)
        own_u.append(dot(acc[mine, :].astype(BF16), wuv[h]))
        m_own = jnp.where(lane == h, top[mine], m_own)
        l_own = jnp.where(lane == h, total[mine], l_own)

    for d in range(2):
        for i, (src, dst) in enumerate(((ml_out, ml_in), (u_out, u_in))):
            pltpu.make_async_remote_copy(
                src_ref=src.at[d], dst_ref=dst.at[d],
                send_sem=usend_sem.at[d, i], recv_sem=urecv_sem.at[d, i],
                device_id={"dp": nxt}, device_id_type=MESH,
            ).wait_recv()

    for copy in c_wo:
        copy.wait()

    ms = [m_own, ml_in[0], ml_in[1]]
    ls = [l_own] + [pltpu.roll(ml_in[d], 128 - n_heads, 1) for d in range(2)]
    peak = jnp.maximum(jnp.maximum(ms[0], ms[1]), ms[2])
    fs = [jnp.where(lane < n_heads, jnp.exp2((m - peak) * SCALE2), 1.0) for m in ms]
    ls = [jnp.where(lane < n_heads, one, 1.0) for one in ls]
    share = 1.0 / (fs[0] * ls[0] + fs[1] * ls[1] + fs[2] * ls[2])
    fs = [f * share for f in fs]
    for h in range(n_heads):
        at = slice(h * VDIM, (h + 1) * VDIM)
        us = [own_u[h], u_in[0, :, at].astype(F32), u_in[1, :, at].astype(F32)]
        gs = [jnp.broadcast_to(f[:, h : h + 1], (reqs, VDIM)) for f in fs]
        heads_out[:, at] = (gs[0] * us[0] + gs[1] * us[1] + gs[2] * us[2]).astype(BF16)

    sends = []
    for p in range(parts):
        y_out[p] = dot(heads_out[...], wo[p]).astype(BF16)
        copy = pltpu.make_async_remote_copy(
            src_ref=y_out.at[p], dst_ref=y_in.at[p],
            send_sem=ysend_sem.at[p], recv_sem=yrecv_sem.at[p],
            device_id={"tp": 1 - side}, device_id_type=MESH,
        )
        copy.start()
        sends.append(copy)
    mine = [dot(heads_out[...], wo[parts + p]) for p in range(parts)]

    for p in range(parts):
        sends[p].wait_recv()
        out_ref[:, p * piece : (p + 1) * piece] = (mine[p] + y_in[p].astype(F32)).astype(BF16)
    for copy in asks + backs + sends:
        copy.wait_send()

def shards(
    n_dp, q_nope, q_rope, lengths, page_table, lend_counts, latent_pages, rope_pages, w_uk, w_uv, w_o
):
    reqs = lengths.shape[0]
    slots, _, latent = latent_pages.shape
    n_heads = w_uk.shape[0]
    half = w_o.shape[1] // 2
    rows = reqs * n_heads
    tokens = slots * PAGE
    vmem = pltpu.VMEM
    dma = pltpu.SemaphoreType.DMA
    return pl.pallas_call(
        functools.partial(kernel, n_dp),
        out_shape=jax.ShapeDtypeStruct((reqs, half), BF16),
        in_specs=[pl.BlockSpec(memory_space=pltpu.HBM)] * 10,
        out_specs=pl.BlockSpec(memory_space=vmem),
        scratch_shapes=[
            vmem(q_nope.shape, BF16),
            vmem(q_rope.shape, BF16),
            vmem((MAXP, reqs), jnp.int32),
            vmem((2, reqs), jnp.int32),
            vmem((1, reqs), jnp.int32),
            vmem((2, 8, 128), jnp.int32),
            vmem((slots, PAGE, latent), BF16),
            vmem(rope_pages.shape, BF16),
            vmem(w_uk.shape, BF16),
            vmem(w_uv.shape, BF16),
            vmem((2 * PARTS, w_o.shape[0], half // PARTS), BF16),
            vmem((2, *q_nope.shape), BF16),
            vmem((2, *q_rope.shape), BF16),
            vmem((2, 8, 128), jnp.int32),
            pltpu.SMEM((2, 8, 128), jnp.int32),
            vmem((512, 256), BF16),
            vmem((slots, PAGE, 128), BF16),
            vmem((rows, latent + 128), BF16),
            vmem((reqs, tokens), F32),
            vmem((rows, tokens), F32),
            vmem((rows, 128), F32),
            vmem((rows, tokens), BF16),
            vmem((rows, latent), F32),
            vmem((latent // 128 + 1, rows, 128), F32),
            vmem((latent // 128, rows, 128), F32),
            vmem((rows, 128), F32),
            vmem((rows, 128), F32),
            vmem((2, reqs, n_heads * VDIM), BF16),
            vmem((2, reqs, 128), F32),
            vmem((2, reqs, n_heads * VDIM), BF16),
            vmem((2, reqs, 128), F32),
            vmem((reqs, n_heads * VDIM), BF16),
            vmem((PARTS, reqs, half // PARTS), BF16),
            vmem((PARTS, reqs, half // PARTS), BF16),
            dma((11 + 2 * PARTS,)),
            dma((2,)),
            dma((2, 3)),
            dma((2, 3)),
            dma((2, 2)),
            dma((2, 2)),
            dma((PARTS,)),
            dma((PARTS,)),
        ],
        compiler_params=pltpu.CompilerParams(
            collective_id=0, has_side_effects=True, vmem_limit_bytes=44 * 1024 * 1024
        ),
        name="latent_step",
    )(
        *(
            pltpu.with_memory_space_constraint(x, pltpu.HBM)
            for x in (
                q_nope, q_rope, page_table.T, lend_counts.T, lengths.reshape(1, reqs),
                latent_pages, rope_pages, w_uk, w_uv, w_o,
            )
        )
    )

def solution(mesh):
    in_specs = (
        P("dp", "tp"),
        P("dp", "tp"),
        P("dp"),
        P("dp", None),
        P("dp", None),
        P("dp", None, None),
        P("dp", None),
        P("tp", None, None),
        P("tp", None, None),
        P("tp", None),
    )
    return jax.shard_map(
        functools.partial(shards, mesh.shape["dp"]),
        mesh=mesh, in_specs=in_specs, out_specs=P("dp", "tp"), check_vma=False,
    )
```

```python
import functools
import math

import jax
import jax.numpy as jnp
from jax import lax
from jax.experimental import pallas as pl
from jax.experimental.pallas import tpu as pltpu
from jax.sharding import PartitionSpec as P

ROPE = 64
NOPE = 128
VDIM = 128
PAGE = 64
MAXP = 8
LEND = 2
MESH = pl.DeviceIdType.MESH
NEG = -3e38
SCALE2 = math.log2(math.e) / math.sqrt(NOPE + ROPE)
GROUP = 8
PARTS = 2
POOL_COPIES = 8
RELAY = 15
F32 = jnp.float32
BF16 = jnp.bfloat16

def dot(a, b):
    return lax.dot_general(a, b, (((1,), (0,)), ((), ())), preferred_element_type=F32)

def dot_t(a, b):
    return lax.dot_general(a, b, (((1,), (1,)), ((), ())), preferred_element_type=F32)

def iota(shape, dim):
    return lax.broadcasted_iota(jnp.int32, shape, dim)

def doubled_rope(q_rope, head):
    pair = q_rope[:, (head // 2) * 128 : (head // 2 + 1) * 128].astype(F32)
    turned = pltpu.roll(pair, 64, 1)
    low = iota(pair.shape, 1) < 64
    return jnp.where(low, pair, turned) if head % 2 == 0 else jnp.where(low, turned, pair)

def kernel(
    n_dp, relay,
    qn_hbm, qr_hbm, table_hbm, lent_hbm, size_hbm, lat_hbm, rope_hbm, wuk_hbm, wuv_hbm, wo_hbm,
    out_ref,
    qn, qr, table, lent, size, plan, lat, rope, wuk, wuv, wo,
    qn_in, qr_in, plan_in, qn_by, qr_by, plan_by, plan_sm,
    perm, keys, q_own, bias, scores, peaks, totals, probs, acc,
    q_far, o_far, m_far, l_far,
    u_out, ml_out, u_in, ml_in, heads_out, y_out, y_in,
    load_sem, sm_sem, gate_sem, bysend_sem, byrecv_sem, qsend_sem, qrecv_sem, usend_sem, urecv_sem, ysend_sem, yrecv_sem,
):
    reqs = qn.shape[0]
    n_heads = wuk.shape[0]
    slots = rope.shape[0]
    latent = lat.shape[2]
    wide = latent // 128
    half = out_ref.shape[1]
    rows = reqs * n_heads
    parts = y_out.shape[0]
    piece = half // parts

    me = lax.axis_index("dp")
    side = lax.axis_index("tp")
    nxt = lax.rem(me + 1, n_dp)
    prv = lax.rem(me + n_dp - 1, n_dp)
    last = n_dp - 1
    near = jnp.where((me == 1) | (me == last), 0, lax.rem(me, 2))

    def local(src, dst, i):
        copy = pltpu.make_async_copy(src, dst, load_sem.at[i])
        copy.start()
        return copy

    barrier = pltpu.get_barrier_semaphore()

    def arrive(**target):
        pl.semaphore_signal(barrier, inc=1, device_id=target, device_id_type=MESH)

    pl.when(me != last)(lambda: arrive(dp=nxt))
    arrive(dp=prv)
    arrive(tp=1 - side)

    @pl.when(me == relay)
    def _():
        arrive(dp=last)
        arrive(dp=0)

    c_table = local(table_hbm, table, 0)
    c_lent = local(lent_hbm, lent, 1)
    c_size = local(size_hbm, size, 2)
    c_rope = local(rope_hbm, rope, 5)
    c_qn = local(qn_hbm, qn, 3)
    c_qr = local(qr_hbm, qr, 4)
    c_wuk = local(wuk_hbm, wuk, 6)
    pool_at = 8 + 2 * parts
    share = slots // POOL_COPIES
    c_lat = [
        local(lat_hbm.at[pl.ds(i * share, share)], lat.at[pl.ds(i * share, share)], pool_at + i)
        for i in range(POOL_COPIES)
    ]

    out_row = iota((512, 256), 0)
    in_row = iota((512, 256), 1)
    hit = ((out_row >> 5) == (in_row & 15)) & (((out_row & 31) >> 1) == (in_row >> 4))
    perm[...] = jnp.where(hit, 1.0, 0.0).astype(BF16)

    c_table.wait()
    c_lent.wait()
    c_size.wait()

    def spread(row):
        return jnp.broadcast_to(row, (8, reqs))

    row8 = iota((8, reqs), 0)
    pages = table[...]
    length = spread(size[...])
    lent_left = spread(lent[0:1, :])
    lent_right = spread(lent[1:2, :])
    n_pages = (length + (PAGE - 1)) >> 6
    first = n_pages - lent_left - lent_right
    for d in range(2):
        start = first if d == 0 else n_pages - lent_right
        held = lent_left if d == 0 else lent_right
        packed = jnp.zeros((8, reqs), jnp.int32)
        for j in range(LEND):
            at = start + j
            slot = spread(jnp.sum(jnp.where(row8 == at, pages, 0), axis=0, keepdims=True))
            used = held > j
            slot = jnp.where(used, jnp.clip(slot, 0, slots - 1), 0)
            live = jnp.where(used, jnp.clip(length - at * PAGE, 0, PAGE), 0)
            packed = jnp.where(row8 == j, slot, packed)
            packed = jnp.where(row8 == LEND + j, live, packed)
        plan[d, :, 0:reqs] = packed

    c_rope.wait()
    row_odd = (iota((512, 128), 0) & 1) == 1
    lane_high = iota((512, 128), 1) >= 64
    keep = row_odd == lane_high
    for g in range(slots // 16):
        page_rows = pl.ds(g * 16, 16)
        left = jnp.concatenate(
            [rope[page_rows, j * 128 : (j + 1) * 128] for j in range(16)], axis=0
        )
        right = jnp.concatenate(
            [rope[page_rows, (16 + j) * 128 : (17 + j) * 128] for j in range(16)], axis=0
        )
        moved = dot(perm[...], jnp.concatenate([left, right], axis=1))
        for s in range(2):
            part = jnp.where(keep, moved[:, s * 128 : (s + 1) * 128], 0.0).astype(BF16)
            keys[page_rows, s * 32 : (s + 1) * 32, :] = part.reshape(16, 32, 128)

    c_qn.wait()
    c_qr.wait()

    def pool_ready():
        c_wuk.wait()
        for copy in c_lat:
            copy.wait()

    def own_scores():
        for h in range(n_heads):
            mine = pl.ds(h * reqs, reqs)
            q_own[mine, 0:latent] = dot(qn[:, h * NOPE : (h + 1) * NOPE], wuk[h]).astype(BF16)
            q_own[mine, latent : latent + 128] = doubled_rope(qr, h).astype(BF16)
        top = None
        for i in range(slots // 4):
            at = i * 4 * PAGE
            s = dot_t(q_own[:, 0:latent], lat[i * 4 : i * 4 + 4].reshape(256, latent))
            s = s + dot_t(
                q_own[:, latent : latent + 128], keys[i * 4 : i * 4 + 4].reshape(256, 128)
            )
            b = bias[:, at : at + 256]
            s = (s.reshape(n_heads, reqs, 256) + b[None]).reshape(rows, 256)
            scores[:, at : at + 256] = s
            peak = jnp.maximum(s[:, 0:128], s[:, 128:256])
            top = peak if top is None else jnp.maximum(top, peak)
        peaks[...] = top

    @pl.when(me == last)
    def _():
        pl.semaphore_wait(barrier, 4)
        pl.semaphore_signal(gate_sem, inc=1, device_id={"dp": relay}, device_id_type=MESH)

    pl.when(me != last)(lambda: pl.semaphore_wait(barrier, 3))

    def ask(d, i, src, dst):
        return pltpu.make_async_remote_copy(
            src_ref=src, dst_ref=dst.at[d],
            send_sem=qsend_sem.at[d, i], recv_sem=qrecv_sem.at[d, i],
            device_id={"dp": prv if isinstance(d, int) and d == 0 else nxt}, device_id_type=MESH,
        )

    asks = []
    for d in range(2):
        asks.append(ask(d, 2, plan.at[d], plan_in))
        asks.append(ask(d, 0, qn, qn_in))
        asks.append(ask(d, 1, qr, qr_in))

    def to_relay(i):
        src, dst = [(qn, qn_by), (qr, qr_by), (plan.at[0], plan_by)][i]
        return pltpu.make_async_remote_copy(
            src_ref=src, dst_ref=dst, send_sem=qsend_sem.at[0, i], recv_sem=byrecv_sem.at[i],
            device_id={"dp": relay}, device_id_type=MESH,
        )

    def from_relay(i):
        src, dst = [(qn_by, qn_in), (qr_by, qr_in), (plan_by, plan_in)][i]
        return pltpu.make_async_remote_copy(
            src_ref=src, dst_ref=dst.at[0], send_sem=bysend_sem.at[i], recv_sem=qrecv_sem.at[0, i],
            device_id={"dp": last}, device_id_type=MESH,
        )

    @pl.when(me == 0)
    def _():
        for i in (2, 0, 1):
            to_relay(i).start()

    @pl.when(me != 0)
    def _():
        for copy in asks[:3]:
            copy.start()

    for copy in asks[3:]:
        copy.start()
    c_wuv = local(wuv_hbm, wuv, 7)
    c_wo = [
        local(
            wo_hbm.at[:, pl.ds((1 - side) * half + p * piece, piece)], wo.at[p], 8 + p
        )
        for p in range(parts)
    ] + [
        local(wo_hbm.at[:, pl.ds(side * half + p * piece, piece)], wo.at[parts + p], 8 + parts + p)
        for p in range(parts)
    ]

    lane = iota((reqs, 128), 1)
    facts = jnp.concatenate([pages, first, length], axis=0).astype(F32)
    facts = jnp.concatenate([facts, jnp.zeros((24, 128 - reqs), F32)], axis=1)
    facts = jnp.concatenate([facts, jnp.zeros((104, 128), F32)], axis=0)
    facts = jnp.transpose(facts)[0:reqs].astype(jnp.int32)

    def column(i):
        return jnp.broadcast_to(facts[:, i : i + 1], (reqs, 128))

    first = column(8)
    length = column(16)
    count = jnp.zeros((reqs, 128), jnp.int32)
    for k in range(MAXP):
        live = jnp.clip(length - k * PAGE, 0, PAGE)
        count = count + jnp.where((lane == column(k)) & (first > k), live, 0)
    for g in range(slots // 2):
        even = jnp.broadcast_to(count[:, 2 * g : 2 * g + 1], (reqs, 128))
        odd = jnp.broadcast_to(count[:, 2 * g + 1 : 2 * g + 2], (reqs, 128))
        limit = jnp.where(lane < 64, even, odd)
        bias[:, g * 128 : (g + 1) * 128] = jnp.where((lane & 63) < limit, 0.0, NEG)

    pool_ready()
    lane8 = iota((8, 128), 1)

    some = n_heads // 2

    def back(d, i, target):
        src, dst = (ml_out, ml_in) if i == 0 else (u_out, u_in)
        src, dst = src.at[d], dst.at[d]
        if i > 0:
            src, dst = src.at[i - 1], dst.at[i - 1]
        return pltpu.make_async_remote_copy(
            src_ref=src, dst_ref=dst,
            send_sem=usend_sem.at[d, i], recv_sem=urecv_sem.at[d, i],
            device_id={"dp": target}, device_id_type=MESH,
        )

    def far_terms(d, wuv_copy):
        ask(d, 2, plan.at[0], plan_in).wait_recv()
        c_sm = pltpu.make_async_copy(plan_in.at[d], plan_sm.at[d], sm_sem.at[d])
        c_sm.start()
        ask(d, 0, qn, qn_in).wait_recv()
        for h in range(n_heads):
            far = dot(qn_in[d, :, h * NOPE : (h + 1) * NOPE], wuk[h])
            at = pl.ds(h, reqs, stride=n_heads)
            for j in range(wide):
                q_far[j, at, :] = far[:, j * 128 : (j + 1) * 128]
        ask(d, 1, qr, qr_in).wait_recv()
        q_rope = qr_in[d]
        for h in range(n_heads):
            q_far[wide, pl.ds(h, reqs, stride=n_heads), :] = doubled_rope(q_rope, h)
        c_sm.wait()

        def held(pair):
            return [
                (plan_sm[d, j, r], plan_sm[d, LEND + j, r])
                for r in (2 * pair, 2 * pair + 1)
                for j in range(LEND)
            ]

        def far_weights(pair):
            found = held(pair)
            at = slice(pair * 16, pair * 16 + 16)
            k_lat = jnp.concatenate([lat[slot] for slot, _ in found], axis=0)
            k_rope = jnp.concatenate([keys[slot] for slot, _ in found], axis=0)
            q_lat = jnp.concatenate([q_far[j, at, :] for j in range(wide)], axis=1).astype(BF16)
            q_rope = q_far[wide, at, :].astype(BF16)
            if pair % 2:
                s = dot_t(k_lat, q_lat) + dot_t(k_rope, q_rope)
                s = jnp.concatenate([s[0:128].T, s[128:256].T], axis=1)
            else:
                s = dot_t(q_lat, k_lat) + dot_t(q_rope, k_rope)
            blocks = []
            for e in range(2):
                limit = jnp.where(lane8 < 64, found[2 * e][1], found[2 * e + 1][1])
                part = s[e * 8 : (e + 1) * 8, e * 128 : (e + 1) * 128]
                part = jnp.where((lane8 & 63) < limit, part, NEG)
                peak = jnp.maximum(jnp.max(part, axis=1, keepdims=True), -1e30)
                w = jnp.exp2((part - peak) * SCALE2)
                total = jnp.sum(w, axis=1, keepdims=True)
                here = slice(pair * 16 + e * 8, pair * 16 + e * 8 + 8)
                m_far[here, :] = jnp.broadcast_to(peak, (8, 128))
                l_far[here, :] = jnp.broadcast_to(total, (8, 128))
                blocks.append(w)
            return blocks

        def far_values(pair, blocks):
            found = held(pair)
            none = jnp.zeros((8, 128), F32)
            w = jnp.concatenate(
                [
                    jnp.concatenate([blocks[0], none], axis=1),
                    jnp.concatenate([none, blocks[1]], axis=1),
                ],
                axis=0,
            ).astype(BF16)
            o = dot(w, jnp.concatenate([lat[slot] for slot, _ in found], axis=0))
            for j in range(wide):
                o_far[j, pair * 16 : pair * 16 + 16, :] = o[:, j * 128 : (j + 1) * 128]

        pairs = reqs // 2
        waiting = {}
        for pair in range(pairs + GROUP):
            if pair < pairs:
                waiting[pair] = far_weights(pair)
            if pair >= GROUP:
                far_values(pair - GROUP, waiting.pop(pair - GROUP))

        backs = []

        def send_back(i):
            copy = back(d, i, jnp.where(d == 0, nxt, prv))
            copy.start()
            backs.append(copy)

        if wuv_copy is not None:

            @pl.when(me == relay)
            def _():
                pl.semaphore_wait(gate_sem, 1)
                for i in (2, 0, 1):
                    to_relay(i).wait_recv()
                    from_relay(i).start()

        pack = jnp.zeros((reqs, 128), F32)
        for h in range(n_heads):
            at = pl.ds(h, reqs, stride=n_heads)
            pack = jnp.where(lane == h, m_far[at, :], pack)
            pack = jnp.where(lane == n_heads + h, l_far[at, :], pack)
        ml_out[d] = pack
        send_back(0)
        if wuv_copy is not None:
            wuv_copy.wait()
        for h in range(n_heads):
            at = pl.ds(h, reqs, stride=n_heads)
            o = jnp.concatenate([o_far[j, at, :] for j in range(wide)], axis=1)
            u = dot(o.astype(BF16), wuv[h]).astype(BF16)
            u_out[d, h // some, :, (h % some) * VDIM : (h % some + 1) * VDIM] = u
            if h % some == some - 1:
                send_back(1 + h // some)
        return backs

    backs = far_terms(near, c_wuv)
    pl.when(me == 0)(own_scores)

    backs += far_terms(1 - near, None)

    pl.when(me != 0)(own_scores)


    top = jnp.max(peaks[...], axis=1, keepdims=True)
    span = 16 * PAGE
    steps = slots // 16
    parts_v = []
    for i in range(steps + 1):
        if i < steps:
            base = top if i < 2 else top + parts_v[i - 2][:, 0:128] * 0.0
            for h in range(n_heads):
                mine = slice(h * reqs, (h + 1) * reqs)
                total = None if i == 0 else totals[mine, :]
                for j in range(span // 128):
                    at = i * span + j * 128
                    w = jnp.exp2((scores[mine, at : at + 128] - base[mine]) * SCALE2)
                    total = w if total is None else total + w
                    probs[mine, at : at + 128] = w.astype(BF16)
                totals[mine, :] = total
        if i > 0:
            k = i - 1
            part = dot(
                probs[:, k * span : (k + 1) * span],
                lat[k * 16 : (k + 1) * 16].reshape(span, latent),
            )
            parts_v.append(part)
            if k == 0:
                acc[:, 0:latent] = part
            else:
                acc[:, 0:latent] += part
    total = jnp.sum(totals[...], axis=1, keepdims=True)

    own_u = []
    m_own = jnp.zeros((reqs, 128), F32)
    l_own = jnp.zeros((reqs, 128), F32)
    for h in range(n_heads):
        mine = slice(h * reqs, (h + 1) * reqs)
        own_u.append(dot(acc[mine, 0:latent].astype(BF16), wuv[h]))
        m_own = jnp.where(lane == h, top[mine], m_own)
        l_own = jnp.where(lane == h, total[mine], l_own)

    for d in range(2):
        for i in range(3):
            back(d, i, nxt).wait_recv()

    for copy in c_wo:
        copy.wait()

    ms = [m_own, ml_in[0], ml_in[1]]
    ls = [l_own] + [pltpu.roll(ml_in[d], 128 - n_heads, 1) for d in range(2)]
    peak = jnp.maximum(jnp.maximum(ms[0], ms[1]), ms[2])
    fs = [jnp.where(lane < n_heads, jnp.exp2((m - peak) * SCALE2), 1.0) for m in ms]
    ls = [jnp.where(lane < n_heads, one, 1.0) for one in ls]
    share = 1.0 / (fs[0] * ls[0] + fs[1] * ls[1] + fs[2] * ls[2])
    fs = [f * share for f in fs]
    for h in range(n_heads):
        at = slice(h * VDIM, (h + 1) * VDIM)
        us = [own_u[h]] + [
            u_in[d, h // some, :, (h % some) * VDIM : (h % some + 1) * VDIM].astype(F32)
            for d in range(2)
        ]
        gs = [jnp.broadcast_to(f[:, h : h + 1], (reqs, VDIM)) for f in fs]
        heads_out[:, at] = (gs[0] * us[0] + gs[1] * us[1] + gs[2] * us[2]).astype(BF16)

    sends = []
    for p in range(parts):
        y_out[p] = dot(heads_out[...], wo[p]).astype(BF16)
        copy = pltpu.make_async_remote_copy(
            src_ref=y_out.at[p], dst_ref=y_in.at[p],
            send_sem=ysend_sem.at[p], recv_sem=yrecv_sem.at[p],
            device_id={"tp": 1 - side}, device_id_type=MESH,
        )
        copy.start()
        sends.append(copy)
    mine = [dot(heads_out[...], wo[parts + p]) for p in range(parts)]

    for p in range(parts):
        sends[p].wait_recv()
        out_ref[:, p * piece : (p + 1) * piece] = (mine[p] + y_in[p].astype(F32)).astype(BF16)
    for copy in asks + backs + sends:
        copy.wait_send()

    @pl.when(me == relay)
    def _():
        for i in range(3):
            from_relay(i).wait_send()

def shards(
    n_dp, q_nope, q_rope, lengths, page_table, lend_counts, latent_pages, rope_pages, w_uk, w_uv, w_o
):
    reqs = lengths.shape[0]
    slots, _, latent = latent_pages.shape
    n_heads = w_uk.shape[0]
    half = w_o.shape[1] // 2
    rows = reqs * n_heads
    tokens = slots * PAGE
    vmem = pltpu.VMEM
    dma = pltpu.SemaphoreType.DMA
    return pl.pallas_call(
        functools.partial(kernel, n_dp, RELAY if n_dp > RELAY + 1 else n_dp // 2),
        out_shape=jax.ShapeDtypeStruct((reqs, half), BF16),
        in_specs=[pl.BlockSpec(memory_space=pltpu.HBM)] * 10,
        out_specs=pl.BlockSpec(memory_space=vmem),
        scratch_shapes=[
            vmem(q_nope.shape, BF16),
            vmem(q_rope.shape, BF16),
            vmem((MAXP, reqs), jnp.int32),
            vmem((2, reqs), jnp.int32),
            vmem((1, reqs), jnp.int32),
            vmem((2, 8, 128), jnp.int32),
            vmem((slots, PAGE, latent), BF16),
            vmem(rope_pages.shape, BF16),
            vmem(w_uk.shape, BF16),
            vmem(w_uv.shape, BF16),
            vmem((2 * PARTS, w_o.shape[0], half // PARTS), BF16),
            vmem((2, *q_nope.shape), BF16),
            vmem((2, *q_rope.shape), BF16),
            vmem((2, 8, 128), jnp.int32),
            vmem(q_nope.shape, BF16),
            vmem(q_rope.shape, BF16),
            vmem((8, 128), jnp.int32),
            pltpu.SMEM((2, 8, 128), jnp.int32),
            vmem((512, 256), BF16),
            vmem((slots, PAGE, 128), BF16),
            vmem((rows, latent + 128), BF16),
            vmem((reqs, tokens), F32),
            vmem((rows, tokens + 128), F32),
            vmem((rows, 128), F32),
            vmem((rows, 128), F32),
            vmem((rows, tokens + 128), BF16),
            vmem((rows, latent + 128), F32),
            vmem((latent // 128 + 1, rows, 128), F32),
            vmem((latent // 128, rows, 128), F32),
            vmem((rows, 128), F32),
            vmem((rows, 128), F32),
            vmem((2, 2, reqs, n_heads // 2 * VDIM), BF16),
            vmem((2, reqs, 128), F32),
            vmem((2, 2, reqs, n_heads // 2 * VDIM), BF16),
            vmem((2, reqs, 128), F32),
            vmem((reqs, n_heads * VDIM), BF16),
            vmem((PARTS, reqs, half // PARTS), BF16),
            vmem((PARTS, reqs, half // PARTS), BF16),
            dma((8 + 2 * PARTS + POOL_COPIES,)),
            dma((2,)),
            pltpu.SemaphoreType.REGULAR,
            dma((3,)),
            dma((3,)),
            dma((2, 3)),
            dma((2, 3)),
            dma((2, 3)),
            dma((2, 3)),
            dma((PARTS,)),
            dma((PARTS,)),
        ],
        compiler_params=pltpu.CompilerParams(
            collective_id=0, has_side_effects=True, vmem_limit_bytes=44 * 1024 * 1024
        ),
        name="latent_step",
    )(
        *(
            pltpu.with_memory_space_constraint(x, pltpu.HBM)
            for x in (
                q_nope, q_rope, page_table.T, lend_counts.T, lengths.reshape(1, reqs),
                latent_pages, rope_pages, w_uk, w_uv, w_o,
            )
        )
    )

def solution(mesh):
    in_specs = (
        P("dp", "tp"),
        P("dp", "tp"),
        P("dp"),
        P("dp", None),
        P("dp", None),
        P("dp", None, None),
        P("dp", None),
        P("tp", None, None),
        P("tp", None, None),
        P("tp", None),
    )
    return jax.shard_map(
        functools.partial(shards, mesh.shape["dp"]),
        mesh=mesh, in_specs=in_specs, out_specs=P("dp", "tp"), check_vma=False,
    )
```

```python
import functools
import math

import jax
import jax.numpy as jnp
from jax import lax
from jax.experimental import pallas as pl
from jax.experimental.pallas import tpu as pltpu
from jax.sharding import PartitionSpec as P

ROPE = 64
NOPE = 128
VDIM = 128
PAGE = 64
MAXP = 8
LEND = 2
MESH = pl.DeviceIdType.MESH
NEG = -3e38
SCALE2 = math.log2(math.e) / math.sqrt(NOPE + ROPE)
GROUP = 8
PARTS = 2
POOL_COPIES = 8
RELAY = 15
F32 = jnp.float32
BF16 = jnp.bfloat16

def dot(a, b):
    return lax.dot_general(a, b, (((1,), (0,)), ((), ())), preferred_element_type=F32)

def dot_t(a, b):
    return lax.dot_general(a, b, (((1,), (1,)), ((), ())), preferred_element_type=F32)

def iota(shape, dim):
    return lax.broadcasted_iota(jnp.int32, shape, dim)

def doubled_rope(q_rope, head):
    pair = q_rope[:, (head // 2) * 128 : (head // 2 + 1) * 128].astype(F32)
    turned = pltpu.roll(pair, 64, 1)
    low = iota(pair.shape, 1) < 64
    return jnp.where(low, pair, turned) if head % 2 == 0 else jnp.where(low, turned, pair)

def kernel(
    n_dp, relay,
    qn_hbm, qr_hbm, table_hbm, lent_hbm, size_hbm, lat_hbm, rope_hbm, wuk_hbm, wuv_hbm, wo_hbm,
    out_ref,
    qn, qr, table, lent, size, plan, lat, rope, wuk, wuv, wo,
    qn_in, qr_in, plan_in, qn_by, qr_by, plan_by, plan_sm,
    perm, keys, q_own, bias, scores, peaks, totals, probs, acc,
    q_far, o_far, m_far, l_far,
    u_out, ml_out, u_in, ml_in, heads_out, y_out, y_in,
    load_sem, sm_sem, gate_sem, bysend_sem, byrecv_sem, qsend_sem, qrecv_sem, usend_sem, urecv_sem, ysend_sem, yrecv_sem,
):
    reqs = qn.shape[0]
    n_heads = wuk.shape[0]
    slots = rope.shape[0]
    latent = lat.shape[2]
    wide = latent // 128
    half = out_ref.shape[1]
    rows = reqs * n_heads
    parts = y_out.shape[0]
    piece = half // parts

    me = lax.axis_index("dp")
    side = lax.axis_index("tp")
    nxt = lax.rem(me + 1, n_dp)
    prv = lax.rem(me + n_dp - 1, n_dp)
    last = n_dp - 1
    near = jnp.where((me == 1) | (me == last), 0, lax.rem(me, 2))

    def local(src, dst, i):
        copy = pltpu.make_async_copy(src, dst, load_sem.at[i])
        copy.start()
        return copy

    barrier = pltpu.get_barrier_semaphore()

    def arrive(**target):
        pl.semaphore_signal(barrier, inc=1, device_id=target, device_id_type=MESH)

    pl.when(me != last)(lambda: arrive(dp=nxt))
    arrive(dp=prv)
    arrive(tp=1 - side)

    @pl.when(me == relay)
    def _():
        arrive(dp=last)
        arrive(dp=0)

    c_table = local(table_hbm, table, 0)
    c_lent = local(lent_hbm, lent, 1)
    c_size = local(size_hbm, size, 2)
    c_rope = local(rope_hbm, rope, 5)
    c_qn = local(qn_hbm, qn, 3)
    c_qr = local(qr_hbm, qr, 4)
    c_wuk = local(wuk_hbm, wuk, 6)
    pool_at = 8 + 2 * parts
    share = slots // POOL_COPIES
    c_lat = [
        local(lat_hbm.at[pl.ds(i * share, share)], lat.at[pl.ds(i * share, share)], pool_at + i)
        for i in range(POOL_COPIES)
    ]

    @pl.when(me == last)
    def _():
        pl.semaphore_wait(barrier, 4)
        pl.semaphore_signal(gate_sem, inc=1, device_id={"dp": relay}, device_id_type=MESH)

    out_row = iota((512, 256), 0)
    in_row = iota((512, 256), 1)
    hit = ((out_row >> 5) == (in_row & 15)) & (((out_row & 31) >> 1) == (in_row >> 4))
    perm[...] = jnp.where(hit, 1.0, 0.0).astype(BF16)

    c_table.wait()
    c_lent.wait()
    c_size.wait()

    def spread(row):
        return jnp.broadcast_to(row, (8, reqs))

    row8 = iota((8, reqs), 0)
    pages = table[...]
    length = spread(size[...])
    lent_left = spread(lent[0:1, :])
    lent_right = spread(lent[1:2, :])
    n_pages = (length + (PAGE - 1)) >> 6
    first = n_pages - lent_left - lent_right
    for d in range(2):
        start = first if d == 0 else n_pages - lent_right
        held = lent_left if d == 0 else lent_right
        packed = jnp.zeros((8, reqs), jnp.int32)
        for j in range(LEND):
            at = start + j
            slot = spread(jnp.sum(jnp.where(row8 == at, pages, 0), axis=0, keepdims=True))
            used = held > j
            slot = jnp.where(used, jnp.clip(slot, 0, slots - 1), 0)
            live = jnp.where(used, jnp.clip(length - at * PAGE, 0, PAGE), 0)
            packed = jnp.where(row8 == j, slot, packed)
            packed = jnp.where(row8 == LEND + j, live, packed)
        plan[d, :, 0:reqs] = packed

    c_rope.wait()
    row_odd = (iota((512, 128), 0) & 1) == 1
    lane_high = iota((512, 128), 1) >= 64
    keep = row_odd == lane_high
    for g in range(slots // 16):
        page_rows = pl.ds(g * 16, 16)
        left = jnp.concatenate(
            [rope[page_rows, j * 128 : (j + 1) * 128] for j in range(16)], axis=0
        )
        right = jnp.concatenate(
            [rope[page_rows, (16 + j) * 128 : (17 + j) * 128] for j in range(16)], axis=0
        )
        moved = dot(perm[...], jnp.concatenate([left, right], axis=1))
        for s in range(2):
            part = jnp.where(keep, moved[:, s * 128 : (s + 1) * 128], 0.0).astype(BF16)
            keys[page_rows, s * 32 : (s + 1) * 32, :] = part.reshape(16, 32, 128)

    c_qn.wait()
    c_qr.wait()

    def own_queries():
        for h in range(n_heads):
            mine = pl.ds(h * reqs, reqs)
            q_own[mine, 0:latent] = dot(qn[:, h * NOPE : (h + 1) * NOPE], wuk[h]).astype(BF16)
            q_own[mine, latent : latent + 128] = doubled_rope(qr, h).astype(BF16)

    def own_scores(begin, end):
        top = None if begin == 0 else peaks[...]
        for i in range(begin, end):
            at = i * 4 * PAGE
            s = dot_t(q_own[:, 0:latent], lat[i * 4 : i * 4 + 4].reshape(256, latent))
            s = s + dot_t(
                q_own[:, latent : latent + 128], keys[i * 4 : i * 4 + 4].reshape(256, 128)
            )
            b = bias[:, at : at + 256]
            s = (s.reshape(n_heads, reqs, 256) + b[None]).reshape(rows, 256)
            scores[:, at : at + 256] = s
            peak = jnp.maximum(s[:, 0:128], s[:, 128:256])
            top = peak if top is None else jnp.maximum(top, peak)
        peaks[...] = top

    def own_values():
        top = jnp.max(peaks[...], axis=1, keepdims=True)
        span = 16 * PAGE
        steps = slots // 16
        parts_v = []
        for i in range(steps + 1):
            if i < steps:
                base = top if i < 2 else top + parts_v[i - 2][:, 0:128] * 0.0
                for h in range(n_heads):
                    mine = slice(h * reqs, (h + 1) * reqs)
                    total = None if i == 0 else totals[mine, :]
                    for j in range(span // 128):
                        at = i * span + j * 128
                        w = jnp.exp2((scores[mine, at : at + 128] - base[mine]) * SCALE2)
                        total = w if total is None else total + w
                        probs[mine, at : at + 128] = w.astype(BF16)
                    totals[mine, :] = total
            if i > 0:
                k = i - 1
                part = dot(
                    probs[:, k * span : (k + 1) * span],
                    lat[k * 16 : (k + 1) * 16].reshape(span, latent),
                )
                parts_v.append(part)
                if k == 0:
                    acc[:, 0:latent] = part
                else:
                    acc[:, 0:latent] += part

    def own_rest():
        own_scores(early, slots // 4)
        own_values()

    early = (3 * (slots // POOL_COPIES)) // 4

    pl.when(me != last)(lambda: pl.semaphore_wait(barrier, 3))

    def ask(d, i, src, dst):
        return pltpu.make_async_remote_copy(
            src_ref=src, dst_ref=dst.at[d],
            send_sem=qsend_sem.at[d, i], recv_sem=qrecv_sem.at[d, i],
            device_id={"dp": prv if isinstance(d, int) and d == 0 else nxt}, device_id_type=MESH,
        )

    asks = []
    for d in range(2):
        asks.append(ask(d, 2, plan.at[d], plan_in))
        asks.append(ask(d, 0, qn, qn_in))
        asks.append(ask(d, 1, qr, qr_in))

    def to_relay(i):
        src, dst = [(qn, qn_by), (qr, qr_by), (plan.at[0], plan_by)][i]
        return pltpu.make_async_remote_copy(
            src_ref=src, dst_ref=dst, send_sem=qsend_sem.at[0, i], recv_sem=byrecv_sem.at[i],
            device_id={"dp": relay}, device_id_type=MESH,
        )

    def from_relay(i):
        src, dst = [(qn_by, qn_in), (qr_by, qr_in), (plan_by, plan_in)][i]
        return pltpu.make_async_remote_copy(
            src_ref=src, dst_ref=dst.at[0], send_sem=bysend_sem.at[i], recv_sem=qrecv_sem.at[0, i],
            device_id={"dp": last}, device_id_type=MESH,
        )

    @pl.when(me == 0)
    def _():
        for i in (2, 0, 1):
            to_relay(i).start()

    def start_asks(d):
        for copy in asks[3 * d : 3 * d + 3]:
            copy.start()

    pl.when((me != 0) & (me != relay + 1))(lambda: start_asks(0))
    pl.when(me != relay - 2)(lambda: start_asks(1))
    c_wuv = local(wuv_hbm, wuv, 7)
    c_wo = [
        local(
            wo_hbm.at[:, pl.ds((1 - side) * half + p * piece, piece)], wo.at[p], 8 + p
        )
        for p in range(parts)
    ] + [
        local(wo_hbm.at[:, pl.ds(side * half + p * piece, piece)], wo.at[parts + p], 8 + parts + p)
        for p in range(parts)
    ]

    lane = iota((reqs, 128), 1)
    facts = jnp.concatenate([pages, first, length], axis=0).astype(F32)
    facts = jnp.concatenate([facts, jnp.zeros((24, 128 - reqs), F32)], axis=1)
    facts = jnp.concatenate([facts, jnp.zeros((104, 128), F32)], axis=0)
    facts = jnp.transpose(facts)[0:reqs].astype(jnp.int32)

    def column(i):
        return jnp.broadcast_to(facts[:, i : i + 1], (reqs, 128))

    first = column(8)
    length = column(16)
    count = jnp.zeros((reqs, 128), jnp.int32)
    for k in range(MAXP):
        live = jnp.clip(length - k * PAGE, 0, PAGE)
        count = count + jnp.where((lane == column(k)) & (first > k), live, 0)
    for g in range(slots // 2):
        even = jnp.broadcast_to(count[:, 2 * g : 2 * g + 1], (reqs, 128))
        odd = jnp.broadcast_to(count[:, 2 * g + 1 : 2 * g + 2], (reqs, 128))
        limit = jnp.where(lane < 64, even, odd)
        bias[:, g * 128 : (g + 1) * 128] = jnp.where((lane & 63) < limit, 0.0, NEG)

    c_wuk.wait()
    for copy in c_lat[:3]:
        copy.wait()
    own_queries()
    own_scores(0, early)
    pl.when(me == relay + 1)(lambda: start_asks(0))
    pl.when(me == relay - 2)(lambda: start_asks(1))
    for copy in c_lat[3:]:
        copy.wait()
    lane8 = iota((8, 128), 1)

    some = n_heads // 2

    def back(d, i, target):
        src, dst = (ml_out, ml_in) if i == 0 else (u_out, u_in)
        src, dst = src.at[d], dst.at[d]
        if i > 0:
            src, dst = src.at[i - 1], dst.at[i - 1]
        return pltpu.make_async_remote_copy(
            src_ref=src, dst_ref=dst,
            send_sem=usend_sem.at[d, i], recv_sem=urecv_sem.at[d, i],
            device_id={"dp": target}, device_id_type=MESH,
        )

    def far_terms(d, wuv_copy):
        ask(d, 2, plan.at[0], plan_in).wait_recv()
        c_sm = pltpu.make_async_copy(plan_in.at[d], plan_sm.at[d], sm_sem.at[d])
        c_sm.start()
        ask(d, 0, qn, qn_in).wait_recv()
        for h in range(n_heads):
            far = dot(qn_in[d, :, h * NOPE : (h + 1) * NOPE], wuk[h])
            at = pl.ds(h, reqs, stride=n_heads)
            for j in range(wide):
                q_far[j, at, :] = far[:, j * 128 : (j + 1) * 128]
        ask(d, 1, qr, qr_in).wait_recv()
        q_rope = qr_in[d]
        for h in range(n_heads):
            q_far[wide, pl.ds(h, reqs, stride=n_heads), :] = doubled_rope(q_rope, h)
        c_sm.wait()

        def held(pair):
            return [
                (plan_sm[d, j, r], plan_sm[d, LEND + j, r])
                for r in (2 * pair, 2 * pair + 1)
                for j in range(LEND)
            ]

        def far_weights(pair):
            found = held(pair)
            at = slice(pair * 16, pair * 16 + 16)
            k_lat = jnp.concatenate([lat[slot] for slot, _ in found], axis=0)
            k_rope = jnp.concatenate([keys[slot] for slot, _ in found], axis=0)
            q_lat = jnp.concatenate([q_far[j, at, :] for j in range(wide)], axis=1).astype(BF16)
            q_rope = q_far[wide, at, :].astype(BF16)
            if pair % 2:
                s = dot_t(k_lat, q_lat) + dot_t(k_rope, q_rope)
                s = jnp.concatenate([s[0:128].T, s[128:256].T], axis=1)
            else:
                s = dot_t(q_lat, k_lat) + dot_t(q_rope, k_rope)
            blocks = []
            for e in range(2):
                limit = jnp.where(lane8 < 64, found[2 * e][1], found[2 * e + 1][1])
                part = s[e * 8 : (e + 1) * 8, e * 128 : (e + 1) * 128]
                part = jnp.where((lane8 & 63) < limit, part, NEG)
                peak = jnp.maximum(jnp.max(part, axis=1, keepdims=True), -1e30)
                w = jnp.exp2((part - peak) * SCALE2)
                total = jnp.sum(w, axis=1, keepdims=True)
                here = slice(pair * 16 + e * 8, pair * 16 + e * 8 + 8)
                m_far[here, :] = jnp.broadcast_to(peak, (8, 128))
                l_far[here, :] = jnp.broadcast_to(total, (8, 128))
                blocks.append(w)
            return blocks

        def far_values(pair, blocks):
            found = held(pair)
            none = jnp.zeros((8, 128), F32)
            w = jnp.concatenate(
                [
                    jnp.concatenate([blocks[0], none], axis=1),
                    jnp.concatenate([none, blocks[1]], axis=1),
                ],
                axis=0,
            ).astype(BF16)
            o = dot(w, jnp.concatenate([lat[slot] for slot, _ in found], axis=0))
            for j in range(wide):
                o_far[j, pair * 16 : pair * 16 + 16, :] = o[:, j * 128 : (j + 1) * 128]

        pairs = reqs // 2
        waiting = {}
        for pair in range(pairs + GROUP):
            if pair < pairs:
                waiting[pair] = far_weights(pair)
            if pair >= GROUP:
                far_values(pair - GROUP, waiting.pop(pair - GROUP))

        backs = []

        def send_back(i):
            copy = back(d, i, jnp.where(d == 0, nxt, prv))
            copy.start()
            backs.append(copy)

        pack = jnp.zeros((reqs, 128), F32)
        for h in range(n_heads):
            at = pl.ds(h, reqs, stride=n_heads)
            pack = jnp.where(lane == h, m_far[at, :], pack)
            pack = jnp.where(lane == n_heads + h, l_far[at, :], pack)
        ml_out[d] = pack
        send_back(0)
        if wuv_copy is not None:
            wuv_copy.wait()
        for h in range(n_heads):
            at = pl.ds(h, reqs, stride=n_heads)
            o = jnp.concatenate([o_far[j, at, :] for j in range(wide)], axis=1)
            u = dot(o.astype(BF16), wuv[h]).astype(BF16)
            u_out[d, h // some, :, (h % some) * VDIM : (h % some + 1) * VDIM] = u
            if h % some == some - 1:
                send_back(1 + h // some)
        return backs

    @pl.when(me == relay)
    def _():
        pl.semaphore_wait(gate_sem, 1)
        for i in (2, 0, 1):
            to_relay(i).wait_recv()
            from_relay(i).start()

    backs = far_terms(near, c_wuv)
    pl.when(me == 0)(own_rest)

    backs += far_terms(1 - near, None)

    pl.when(me != 0)(own_rest)

    top = jnp.max(peaks[...], axis=1, keepdims=True)
    total = jnp.sum(totals[...], axis=1, keepdims=True)

    own_u = []
    m_own = jnp.zeros((reqs, 128), F32)
    l_own = jnp.zeros((reqs, 128), F32)
    for h in range(n_heads):
        mine = slice(h * reqs, (h + 1) * reqs)
        own_u.append(dot(acc[mine, 0:latent].astype(BF16), wuv[h]))
        m_own = jnp.where(lane == h, top[mine], m_own)
        l_own = jnp.where(lane == h, total[mine], l_own)

    for d in range(2):
        for i in range(3):
            back(d, i, nxt).wait_recv()

    for copy in c_wo:
        copy.wait()

    ms = [m_own, ml_in[0], ml_in[1]]
    ls = [l_own] + [pltpu.roll(ml_in[d], 128 - n_heads, 1) for d in range(2)]
    peak = jnp.maximum(jnp.maximum(ms[0], ms[1]), ms[2])
    fs = [jnp.where(lane < n_heads, jnp.exp2((m - peak) * SCALE2), 1.0) for m in ms]
    ls = [jnp.where(lane < n_heads, one, 1.0) for one in ls]
    share = 1.0 / (fs[0] * ls[0] + fs[1] * ls[1] + fs[2] * ls[2])
    fs = [f * share for f in fs]
    for h in range(n_heads):
        at = slice(h * VDIM, (h + 1) * VDIM)
        us = [own_u[h]] + [
            u_in[d, h // some, :, (h % some) * VDIM : (h % some + 1) * VDIM].astype(F32)
            for d in range(2)
        ]
        gs = [jnp.broadcast_to(f[:, h : h + 1], (reqs, VDIM)) for f in fs]
        heads_out[:, at] = (gs[0] * us[0] + gs[1] * us[1] + gs[2] * us[2]).astype(BF16)

    sends = []
    for p in range(parts):
        y_out[p] = dot(heads_out[...], wo[p]).astype(BF16)
        copy = pltpu.make_async_remote_copy(
            src_ref=y_out.at[p], dst_ref=y_in.at[p],
            send_sem=ysend_sem.at[p], recv_sem=yrecv_sem.at[p],
            device_id={"tp": 1 - side}, device_id_type=MESH,
        )
        copy.start()
        sends.append(copy)
    mine = [dot(heads_out[...], wo[parts + p]) for p in range(parts)]

    for p in range(parts):
        sends[p].wait_recv()
        out_ref[:, p * piece : (p + 1) * piece] = (mine[p] + y_in[p].astype(F32)).astype(BF16)
    for copy in asks + backs + sends:
        copy.wait_send()

    @pl.when(me == relay)
    def _():
        for i in range(3):
            from_relay(i).wait_send()

def shards(
    n_dp, q_nope, q_rope, lengths, page_table, lend_counts, latent_pages, rope_pages, w_uk, w_uv, w_o
):
    reqs = lengths.shape[0]
    slots, _, latent = latent_pages.shape
    n_heads = w_uk.shape[0]
    half = w_o.shape[1] // 2
    rows = reqs * n_heads
    tokens = slots * PAGE
    vmem = pltpu.VMEM
    dma = pltpu.SemaphoreType.DMA
    return pl.pallas_call(
        functools.partial(kernel, n_dp, RELAY if n_dp > RELAY + 1 else n_dp // 2),
        out_shape=jax.ShapeDtypeStruct((reqs, half), BF16),
        in_specs=[pl.BlockSpec(memory_space=pltpu.HBM)] * 10,
        out_specs=pl.BlockSpec(memory_space=vmem),
        scratch_shapes=[
            vmem(q_nope.shape, BF16),
            vmem(q_rope.shape, BF16),
            vmem((MAXP, reqs), jnp.int32),
            vmem((2, reqs), jnp.int32),
            vmem((1, reqs), jnp.int32),
            vmem((2, 8, 128), jnp.int32),
            vmem((slots, PAGE, latent), BF16),
            vmem(rope_pages.shape, BF16),
            vmem(w_uk.shape, BF16),
            vmem(w_uv.shape, BF16),
            vmem((2 * PARTS, w_o.shape[0], half // PARTS), BF16),
            vmem((2, *q_nope.shape), BF16),
            vmem((2, *q_rope.shape), BF16),
            vmem((2, 8, 128), jnp.int32),
            vmem(q_nope.shape, BF16),
            vmem(q_rope.shape, BF16),
            vmem((8, 128), jnp.int32),
            pltpu.SMEM((2, 8, 128), jnp.int32),
            vmem((512, 256), BF16),
            vmem((slots, PAGE, 128), BF16),
            vmem((rows, latent + 128), BF16),
            vmem((reqs, tokens), F32),
            vmem((rows, tokens + 128), F32),
            vmem((rows, 128), F32),
            vmem((rows, 128), F32),
            vmem((rows, tokens + 128), BF16),
            vmem((rows, latent + 128), F32),
            vmem((latent // 128 + 1, rows, 128), F32),
            vmem((latent // 128, rows, 128), F32),
            vmem((rows, 128), F32),
            vmem((rows, 128), F32),
            vmem((2, 2, reqs, n_heads // 2 * VDIM), BF16),
            vmem((2, reqs, 128), F32),
            vmem((2, 2, reqs, n_heads // 2 * VDIM), BF16),
            vmem((2, reqs, 128), F32),
            vmem((reqs, n_heads * VDIM), BF16),
            vmem((PARTS, reqs, half // PARTS), BF16),
            vmem((PARTS, reqs, half // PARTS), BF16),
            dma((8 + 2 * PARTS + POOL_COPIES,)),
            dma((2,)),
            pltpu.SemaphoreType.REGULAR,
            dma((3,)),
            dma((3,)),
            dma((2, 3)),
            dma((2, 3)),
            dma((2, 3)),
            dma((2, 3)),
            dma((PARTS,)),
            dma((PARTS,)),
        ],
        compiler_params=pltpu.CompilerParams(
            collective_id=0, has_side_effects=True, vmem_limit_bytes=44 * 1024 * 1024
        ),
        name="latent_step",
    )(
        *(
            pltpu.with_memory_space_constraint(x, pltpu.HBM)
            for x in (
                q_nope, q_rope, page_table.T, lend_counts.T, lengths.reshape(1, reqs),
                latent_pages, rope_pages, w_uk, w_uv, w_o,
            )
        )
    )

def solution(mesh):
    in_specs = (
        P("dp", "tp"),
        P("dp", "tp"),
        P("dp"),
        P("dp", None),
        P("dp", None),
        P("dp", None, None),
        P("dp", None),
        P("tp", None, None),
        P("tp", None, None),
        P("tp", None),
    )
    return jax.shard_map(
        functools.partial(shards, mesh.shape["dp"]),
        mesh=mesh, in_specs=in_specs, out_specs=P("dp", "tp"), check_vma=False,
    )
```

```python
import functools
import math

import jax
import jax.numpy as jnp
from jax import lax
from jax.experimental import pallas as pl
from jax.experimental.pallas import tpu as pltpu
from jax.sharding import PartitionSpec as P

ROPE = 64
NOPE = 128
VDIM = 128
PAGE = 64
MAXP = 8
LEND = 2
MESH = pl.DeviceIdType.MESH
NEG = -3e38
SCALE2 = math.log2(math.e) / math.sqrt(NOPE + ROPE)
GROUP = 8
PARTS = 2
POOL_COPIES = 8
RELAY = 15
F32 = jnp.float32
BF16 = jnp.bfloat16

def dot(a, b):
    return lax.dot_general(a, b, (((1,), (0,)), ((), ())), preferred_element_type=F32)

def dot_t(a, b):
    return lax.dot_general(a, b, (((1,), (1,)), ((), ())), preferred_element_type=F32)

def iota(shape, dim):
    return lax.broadcasted_iota(jnp.int32, shape, dim)

def doubled_rope(q_rope, head):
    pair = q_rope[:, (head // 2) * 128 : (head // 2 + 1) * 128].astype(F32)
    turned = pltpu.roll(pair, 64, 1)
    low = iota(pair.shape, 1) < 64
    return jnp.where(low, pair, turned) if head % 2 == 0 else jnp.where(low, turned, pair)

def kernel(
    n_dp, relay,
    qn_hbm, qr_hbm, table_hbm, lent_hbm, size_hbm, lat_hbm, rope_hbm, wuk_hbm, wuv_hbm, wo_hbm,
    out_ref,
    qn, qr, table, lent, size, plan, lat, rope, wuk, wuv, wo,
    qn_in, qr_in, plan_in, qn_by, qr_by, plan_by, plan_sm,
    perm, keys, q_own, bias, scores, peaks, totals, probs, acc,
    q_far, o_far, m_far, l_far,
    u_out, ml_out, u_in, ml_in, heads_out, y_out, y_in,
    load_sem, sm_sem, gate_sem, bysend_sem, byrecv_sem, qsend_sem, qrecv_sem, usend_sem, urecv_sem, ysend_sem, yrecv_sem,
):
    reqs = qn.shape[0]
    n_heads = wuk.shape[0]
    slots = rope.shape[0]
    latent = lat.shape[2]
    wide = latent // 128
    half = out_ref.shape[1]
    rows = reqs * n_heads
    parts = y_out.shape[0]
    piece = half // parts

    me = lax.axis_index("dp")
    side = lax.axis_index("tp")
    nxt = lax.rem(me + 1, n_dp)
    prv = lax.rem(me + n_dp - 1, n_dp)
    last = n_dp - 1
    near = jnp.where((me == 1) | (me == last), 0, lax.rem(me, 2))

    def local(src, dst, i):
        copy = pltpu.make_async_copy(src, dst, load_sem.at[i])
        copy.start()
        return copy

    barrier = pltpu.get_barrier_semaphore()

    def arrive(**target):
        pl.semaphore_signal(barrier, inc=1, device_id=target, device_id_type=MESH)

    pl.when(me != last)(lambda: arrive(dp=nxt))
    arrive(dp=prv)
    arrive(tp=1 - side)

    @pl.when(me == relay)
    def _():
        arrive(dp=last)
        arrive(dp=0)

    c_table = local(table_hbm, table, 0)
    c_lent = local(lent_hbm, lent, 1)
    c_size = local(size_hbm, size, 2)
    c_rope = local(rope_hbm, rope, 5)
    c_qn = local(qn_hbm, qn, 3)
    c_qr = local(qr_hbm, qr, 4)
    c_wuk = local(wuk_hbm, wuk, 6)
    pool_at = 8 + 2 * parts
    share = slots // POOL_COPIES
    c_lat = [
        local(lat_hbm.at[pl.ds(i * share, share)], lat.at[pl.ds(i * share, share)], pool_at + i)
        for i in range(POOL_COPIES)
    ]

    @pl.when(me == last)
    def _():
        pl.semaphore_wait(barrier, 4)
        pl.semaphore_signal(gate_sem, inc=1, device_id={"dp": relay}, device_id_type=MESH)

    out_row = iota((512, 256), 0)
    in_row = iota((512, 256), 1)
    hit = ((out_row >> 5) == (in_row & 15)) & (((out_row & 31) >> 1) == (in_row >> 4))
    perm[...] = jnp.where(hit, 1.0, 0.0).astype(BF16)

    c_table.wait()
    c_lent.wait()
    c_size.wait()

    def spread(row):
        return jnp.broadcast_to(row, (8, reqs))

    row8 = iota((8, reqs), 0)
    pages = table[...]
    length = spread(size[...])
    lent_left = spread(lent[0:1, :])
    lent_right = spread(lent[1:2, :])
    n_pages = (length + (PAGE - 1)) >> 6
    first = n_pages - lent_left - lent_right
    for d in range(2):
        start = first if d == 0 else n_pages - lent_right
        held = lent_left if d == 0 else lent_right
        packed = jnp.zeros((8, reqs), jnp.int32)
        for j in range(LEND):
            at = start + j
            slot = spread(jnp.sum(jnp.where(row8 == at, pages, 0), axis=0, keepdims=True))
            used = held > j
            slot = jnp.where(used, jnp.clip(slot, 0, slots - 1), 0)
            live = jnp.where(used, jnp.clip(length - at * PAGE, 0, PAGE), 0)
            packed = jnp.where(row8 == j, slot, packed)
            packed = jnp.where(row8 == LEND + j, live, packed)
        plan[d, :, 0:reqs] = packed

    lane = iota((reqs, 128), 1)
    facts = jnp.concatenate([pages, first, length], axis=0).astype(F32)
    facts = jnp.concatenate([facts, jnp.zeros((24, 128 - reqs), F32)], axis=1)
    facts = jnp.concatenate([facts, jnp.zeros((104, 128), F32)], axis=0)
    facts = jnp.transpose(facts)[0:reqs].astype(jnp.int32)

    def column(i):
        return jnp.broadcast_to(facts[:, i : i + 1], (reqs, 128))

    first = column(8)
    length = column(16)
    count = jnp.zeros((reqs, 128), jnp.int32)
    for k in range(MAXP):
        live = jnp.clip(length - k * PAGE, 0, PAGE)
        count = count + jnp.where((lane == column(k)) & (first > k), live, 0)
    for g in range(slots // 2):
        even = jnp.broadcast_to(count[:, 2 * g : 2 * g + 1], (reqs, 128))
        odd = jnp.broadcast_to(count[:, 2 * g + 1 : 2 * g + 2], (reqs, 128))
        limit = jnp.where(lane < 64, even, odd)
        bias[:, g * 128 : (g + 1) * 128] = jnp.where((lane & 63) < limit, 0.0, NEG)

    c_rope.wait()
    row_odd = (iota((512, 128), 0) & 1) == 1
    lane_high = iota((512, 128), 1) >= 64
    keep = row_odd == lane_high
    for g in range(slots // 16):
        page_rows = pl.ds(g * 16, 16)
        left = jnp.concatenate(
            [rope[page_rows, j * 128 : (j + 1) * 128] for j in range(16)], axis=0
        )
        right = jnp.concatenate(
            [rope[page_rows, (16 + j) * 128 : (17 + j) * 128] for j in range(16)], axis=0
        )
        moved = dot(perm[...], jnp.concatenate([left, right], axis=1))
        for s in range(2):
            part = jnp.where(keep, moved[:, s * 128 : (s + 1) * 128], 0.0).astype(BF16)
            keys[page_rows, s * 32 : (s + 1) * 32, :] = part.reshape(16, 32, 128)

    c_qn.wait()
    c_qr.wait()

    def own_queries():
        for h in range(n_heads):
            mine = pl.ds(h * reqs, reqs)
            q_own[mine, 0:latent] = dot(qn[:, h * NOPE : (h + 1) * NOPE], wuk[h]).astype(BF16)
            q_own[mine, latent : latent + 128] = doubled_rope(qr, h).astype(BF16)

    def own_scores(begin, end):
        top = None if begin == 0 else peaks[...]
        for i in range(begin, end):
            at = i * 4 * PAGE
            s = dot_t(q_own[:, 0:latent], lat[i * 4 : i * 4 + 4].reshape(256, latent))
            s = s + dot_t(
                q_own[:, latent : latent + 128], keys[i * 4 : i * 4 + 4].reshape(256, 128)
            )
            b = bias[:, at : at + 256]
            s = (s.reshape(n_heads, reqs, 256) + b[None]).reshape(rows, 256)
            scores[:, at : at + 256] = s
            peak = jnp.maximum(s[:, 0:128], s[:, 128:256])
            top = peak if top is None else jnp.maximum(top, peak)
        peaks[...] = top

    def own_values():
        top = jnp.max(peaks[...], axis=1, keepdims=True)
        span = 16 * PAGE
        steps = slots // 16
        parts_v = []
        for i in range(steps + 1):
            if i < steps:
                base = top if i < 2 else top + parts_v[i - 2][:, 0:128] * 0.0
                for h in range(n_heads):
                    mine = slice(h * reqs, (h + 1) * reqs)
                    total = None if i == 0 else totals[mine, :]
                    for j in range(span // 128):
                        at = i * span + j * 128
                        w = jnp.exp2((scores[mine, at : at + 128] - base[mine]) * SCALE2)
                        total = w if total is None else total + w
                        probs[mine, at : at + 128] = w.astype(BF16)
                    totals[mine, :] = total
            if i > 0:
                k = i - 1
                part = dot(
                    probs[:, k * span : (k + 1) * span],
                    lat[k * 16 : (k + 1) * 16].reshape(span, latent),
                )
                parts_v.append(part)
                if k == 0:
                    acc[:, 0:latent] = part
                else:
                    acc[:, 0:latent] += part

    def own_rest():
        own_scores(early, slots // 4)
        own_values()

    early = (3 * (slots // POOL_COPIES)) // 4

    pl.when(me != last)(lambda: pl.semaphore_wait(barrier, 3))

    def ask(d, i, src, dst):
        return pltpu.make_async_remote_copy(
            src_ref=src, dst_ref=dst.at[d],
            send_sem=qsend_sem.at[d, i], recv_sem=qrecv_sem.at[d, i],
            device_id={"dp": prv if isinstance(d, int) and d == 0 else nxt}, device_id_type=MESH,
        )

    asks = []
    for d in range(2):
        asks.append(ask(d, 2, plan.at[d], plan_in))
        asks.append(ask(d, 0, qn, qn_in))
        asks.append(ask(d, 1, qr, qr_in))

    low = reqs // 2
    relayed = ((2, 0), (0, 0), (0, 1), (1, 0), (1, 1))

    def part(ref, i, e):
        return ref if i == 2 else ref.at[pl.ds(e * low, low)]

    def to_relay(i, e):
        src, dst = [(qn, qn_by), (qr, qr_by), (plan.at[0], plan_by)][i]
        return pltpu.make_async_remote_copy(
            src_ref=part(src, i, e), dst_ref=part(dst, i, e),
            send_sem=qsend_sem.at[0, i], recv_sem=byrecv_sem.at[i, e],
            device_id={"dp": relay}, device_id_type=MESH,
        )

    def from_relay(i, e):
        src, dst = [(qn_by, qn_in), (qr_by, qr_in), (plan_by, plan_in)][i]
        return pltpu.make_async_remote_copy(
            src_ref=part(src, i, e), dst_ref=part(dst.at[0], i, e),
            send_sem=bysend_sem.at[i, e], recv_sem=qrecv_sem.at[0, i],
            device_id={"dp": last}, device_id_type=MESH,
        )

    @pl.when(me == 0)
    def _():
        for i, e in relayed:
            to_relay(i, e).start()

    def start_asks(d):
        for copy in asks[3 * d : 3 * d + 3]:
            copy.start()

    pl.when((me != 0) & (me != relay + 1))(lambda: start_asks(0))
    pl.when(me != relay - 2)(lambda: start_asks(1))
    c_wuv = local(wuv_hbm, wuv, 7)
    c_wo = [
        local(
            wo_hbm.at[:, pl.ds((1 - side) * half + p * piece, piece)], wo.at[p], 8 + p
        )
        for p in range(parts)
    ] + [
        local(wo_hbm.at[:, pl.ds(side * half + p * piece, piece)], wo.at[parts + p], 8 + parts + p)
        for p in range(parts)
    ]

    c_wuk.wait()
    for copy in c_lat[:3]:
        copy.wait()
    own_queries()
    own_scores(0, early)
    pl.when(me == relay + 1)(lambda: start_asks(0))
    pl.when(me == relay - 2)(lambda: start_asks(1))
    for copy in c_lat[3:]:
        copy.wait()
    lane8 = iota((8, 128), 1)

    some = n_heads // 2

    def back(d, i, target):
        src, dst = (ml_out, ml_in) if i == 0 else (u_out, u_in)
        src, dst = src.at[d], dst.at[d]
        if i > 0:
            src, dst = src.at[i - 1], dst.at[i - 1]
        return pltpu.make_async_remote_copy(
            src_ref=src, dst_ref=dst,
            send_sem=usend_sem.at[d, i], recv_sem=urecv_sem.at[d, i],
            device_id={"dp": target}, device_id_type=MESH,
        )

    def far_terms(d, wuv_copy):
        ask(d, 2, plan.at[0], plan_in).wait_recv()
        c_sm = pltpu.make_async_copy(plan_in.at[d], plan_sm.at[d], sm_sem.at[d])
        c_sm.start()
        ask(d, 0, qn, qn_in).wait_recv()
        for h in range(n_heads):
            far = dot(qn_in[d, :, h * NOPE : (h + 1) * NOPE], wuk[h])
            at = pl.ds(h, reqs, stride=n_heads)
            for j in range(wide):
                q_far[j, at, :] = far[:, j * 128 : (j + 1) * 128]
        ask(d, 1, qr, qr_in).wait_recv()
        q_rope = qr_in[d]
        for h in range(n_heads):
            q_far[wide, pl.ds(h, reqs, stride=n_heads), :] = doubled_rope(q_rope, h)
        c_sm.wait()

        def held(pair):
            return [
                (plan_sm[d, j, r], plan_sm[d, LEND + j, r])
                for r in (2 * pair, 2 * pair + 1)
                for j in range(LEND)
            ]

        def far_weights(pair):
            found = held(pair)
            at = slice(pair * 16, pair * 16 + 16)
            k_lat = jnp.concatenate([lat[slot] for slot, _ in found], axis=0)
            k_rope = jnp.concatenate([keys[slot] for slot, _ in found], axis=0)
            q_lat = jnp.concatenate([q_far[j, at, :] for j in range(wide)], axis=1).astype(BF16)
            q_rope = q_far[wide, at, :].astype(BF16)
            if pair % 2:
                s = dot_t(k_lat, q_lat) + dot_t(k_rope, q_rope)
                s = jnp.concatenate([s[0:128].T, s[128:256].T], axis=1)
            else:
                s = dot_t(q_lat, k_lat) + dot_t(q_rope, k_rope)
            blocks = []
            for e in range(2):
                limit = jnp.where(lane8 < 64, found[2 * e][1], found[2 * e + 1][1])
                part = s[e * 8 : (e + 1) * 8, e * 128 : (e + 1) * 128]
                part = jnp.where((lane8 & 63) < limit, part, NEG)
                peak = jnp.maximum(jnp.max(part, axis=1, keepdims=True), -1e30)
                w = jnp.exp2((part - peak) * SCALE2)
                total = jnp.sum(w, axis=1, keepdims=True)
                here = slice(pair * 16 + e * 8, pair * 16 + e * 8 + 8)
                m_far[here, :] = jnp.broadcast_to(peak, (8, 128))
                l_far[here, :] = jnp.broadcast_to(total, (8, 128))
                blocks.append(w)
            return blocks

        def far_values(pair, blocks):
            found = held(pair)
            none = jnp.zeros((8, 128), F32)
            w = jnp.concatenate(
                [
                    jnp.concatenate([blocks[0], none], axis=1),
                    jnp.concatenate([none, blocks[1]], axis=1),
                ],
                axis=0,
            ).astype(BF16)
            o = dot(w, jnp.concatenate([lat[slot] for slot, _ in found], axis=0))
            for j in range(wide):
                o_far[j, pair * 16 : pair * 16 + 16, :] = o[:, j * 128 : (j + 1) * 128]

        pairs = reqs // 2
        waiting = {}
        for pair in range(pairs + GROUP):
            if pair < pairs:
                waiting[pair] = far_weights(pair)
            if pair >= GROUP:
                far_values(pair - GROUP, waiting.pop(pair - GROUP))

        backs = []

        def send_back(i):
            copy = back(d, i, jnp.where(d == 0, nxt, prv))
            copy.start()
            backs.append(copy)

        pack = jnp.zeros((reqs, 128), F32)
        for h in range(n_heads):
            at = pl.ds(h, reqs, stride=n_heads)
            pack = jnp.where(lane == h, m_far[at, :], pack)
            pack = jnp.where(lane == n_heads + h, l_far[at, :], pack)
        ml_out[d] = pack
        send_back(0)
        if wuv_copy is not None:
            wuv_copy.wait()
        for h in range(n_heads):
            at = pl.ds(h, reqs, stride=n_heads)
            o = jnp.concatenate([o_far[j, at, :] for j in range(wide)], axis=1)
            u = dot(o.astype(BF16), wuv[h]).astype(BF16)
            u_out[d, h // some, :, (h % some) * VDIM : (h % some + 1) * VDIM] = u
            if h % some == some - 1:
                send_back(1 + h // some)
        return backs

    @pl.when(me == relay)
    def _():
        pl.semaphore_wait(gate_sem, 1)
        for i, e in relayed:
            to_relay(i, e).wait_recv()
            from_relay(i, e).start()

    backs = far_terms(near, c_wuv)
    pl.when(me == 0)(own_rest)

    backs += far_terms(1 - near, None)

    pl.when(me != 0)(own_rest)

    top = jnp.max(peaks[...], axis=1, keepdims=True)
    total = jnp.sum(totals[...], axis=1, keepdims=True)

    own_u = []
    m_own = jnp.zeros((reqs, 128), F32)
    l_own = jnp.zeros((reqs, 128), F32)
    for h in range(n_heads):
        mine = slice(h * reqs, (h + 1) * reqs)
        own_u.append(dot(acc[mine, 0:latent].astype(BF16), wuv[h]))
        m_own = jnp.where(lane == h, top[mine], m_own)
        l_own = jnp.where(lane == h, total[mine], l_own)

    for d in range(2):
        for i in range(3):
            back(d, i, nxt).wait_recv()

    for copy in c_wo:
        copy.wait()

    ms = [m_own, ml_in[0], ml_in[1]]
    ls = [l_own] + [pltpu.roll(ml_in[d], 128 - n_heads, 1) for d in range(2)]
    peak = jnp.maximum(jnp.maximum(ms[0], ms[1]), ms[2])
    fs = [jnp.where(lane < n_heads, jnp.exp2((m - peak) * SCALE2), 1.0) for m in ms]
    ls = [jnp.where(lane < n_heads, one, 1.0) for one in ls]
    share = 1.0 / (fs[0] * ls[0] + fs[1] * ls[1] + fs[2] * ls[2])
    fs = [f * share for f in fs]
    for h in range(n_heads):
        at = slice(h * VDIM, (h + 1) * VDIM)
        us = [own_u[h]] + [
            u_in[d, h // some, :, (h % some) * VDIM : (h % some + 1) * VDIM].astype(F32)
            for d in range(2)
        ]
        gs = [jnp.broadcast_to(f[:, h : h + 1], (reqs, VDIM)) for f in fs]
        heads_out[:, at] = (gs[0] * us[0] + gs[1] * us[1] + gs[2] * us[2]).astype(BF16)

    sends = []
    for p in range(parts):
        y_out[p] = dot(heads_out[...], wo[p]).astype(BF16)
        copy = pltpu.make_async_remote_copy(
            src_ref=y_out.at[p], dst_ref=y_in.at[p],
            send_sem=ysend_sem.at[p], recv_sem=yrecv_sem.at[p],
            device_id={"tp": 1 - side}, device_id_type=MESH,
        )
        copy.start()
        sends.append(copy)
    mine = [dot(heads_out[...], wo[parts + p]) for p in range(parts)]

    for p in range(parts):
        sends[p].wait_recv()
        out_ref[:, p * piece : (p + 1) * piece] = (mine[p] + y_in[p].astype(F32)).astype(BF16)
    for copy in asks + backs + sends:
        copy.wait_send()

    @pl.when(me == relay)
    def _():
        for i, e in relayed:
            from_relay(i, e).wait_send()

def shards(
    n_dp, q_nope, q_rope, lengths, page_table, lend_counts, latent_pages, rope_pages, w_uk, w_uv, w_o
):
    reqs = lengths.shape[0]
    slots, _, latent = latent_pages.shape
    n_heads = w_uk.shape[0]
    half = w_o.shape[1] // 2
    rows = reqs * n_heads
    tokens = slots * PAGE
    vmem = pltpu.VMEM
    dma = pltpu.SemaphoreType.DMA
    return pl.pallas_call(
        functools.partial(kernel, n_dp, RELAY if n_dp > RELAY + 1 else n_dp // 2),
        out_shape=jax.ShapeDtypeStruct((reqs, half), BF16),
        in_specs=[pl.BlockSpec(memory_space=pltpu.HBM)] * 10,
        out_specs=pl.BlockSpec(memory_space=vmem),
        scratch_shapes=[
            vmem(q_nope.shape, BF16),
            vmem(q_rope.shape, BF16),
            vmem((MAXP, reqs), jnp.int32),
            vmem((2, reqs), jnp.int32),
            vmem((1, reqs), jnp.int32),
            vmem((2, 8, 128), jnp.int32),
            vmem((slots, PAGE, latent), BF16),
            vmem(rope_pages.shape, BF16),
            vmem(w_uk.shape, BF16),
            vmem(w_uv.shape, BF16),
            vmem((2 * PARTS, w_o.shape[0], half // PARTS), BF16),
            vmem((2, *q_nope.shape), BF16),
            vmem((2, *q_rope.shape), BF16),
            vmem((2, 8, 128), jnp.int32),
            vmem(q_nope.shape, BF16),
            vmem(q_rope.shape, BF16),
            vmem((8, 128), jnp.int32),
            pltpu.SMEM((2, 8, 128), jnp.int32),
            vmem((512, 256), BF16),
            vmem((slots, PAGE, 128), BF16),
            vmem((rows, latent + 128), BF16),
            vmem((reqs, tokens), F32),
            vmem((rows, tokens + 128), F32),
            vmem((rows, 128), F32),
            vmem((rows, 128), F32),
            vmem((rows, tokens + 128), BF16),
            vmem((rows, latent + 128), F32),
            vmem((latent // 128 + 1, rows, 128), F32),
            vmem((latent // 128, rows, 128), F32),
            vmem((rows, 128), F32),
            vmem((rows, 128), F32),
            vmem((2, 2, reqs, n_heads // 2 * VDIM), BF16),
            vmem((2, reqs, 128), F32),
            vmem((2, 2, reqs, n_heads // 2 * VDIM), BF16),
            vmem((2, reqs, 128), F32),
            vmem((reqs, n_heads * VDIM), BF16),
            vmem((PARTS, reqs, half // PARTS), BF16),
            vmem((PARTS, reqs, half // PARTS), BF16),
            dma((8 + 2 * PARTS + POOL_COPIES,)),
            dma((2,)),
            pltpu.SemaphoreType.REGULAR,
            dma((3, 2)),
            dma((3, 2)),
            dma((2, 3)),
            dma((2, 3)),
            dma((2, 3)),
            dma((2, 3)),
            dma((PARTS,)),
            dma((PARTS,)),
        ],
        compiler_params=pltpu.CompilerParams(
            collective_id=0, has_side_effects=True, vmem_limit_bytes=44 * 1024 * 1024
        ),
        name="latent_step",
    )(
        *(
            pltpu.with_memory_space_constraint(x, pltpu.HBM)
            for x in (
                q_nope, q_rope, page_table.T, lend_counts.T, lengths.reshape(1, reqs),
                latent_pages, rope_pages, w_uk, w_uv, w_o,
            )
        )
    )

def solution(mesh):
    in_specs = (
        P("dp", "tp"),
        P("dp", "tp"),
        P("dp"),
        P("dp", None),
        P("dp", None),
        P("dp", None, None),
        P("dp", None),
        P("tp", None, None),
        P("tp", None, None),
        P("tp", None),
    )
    return jax.shard_map(
        functools.partial(shards, mesh.shape["dp"]),
        mesh=mesh, in_specs=in_specs, out_specs=P("dp", "tp"), check_vma=False,
    )
```
